32 devices in a mesh: win: 2 (over y), dx: 4 (over z), dy: 2 (over x), dz: 2 (over core).
Axes of the slice: x: 2, y: 2, z: 4, core: 2. Of those that a mesh axis runs over, the one named last changes fastest.
Arguments:
- fraction: float32 [3, 8, 2, 2, 768], P(None, ('win', 'dx'), 'dy', 'dz'), parts along dimension 1, may hold values from 0 to 1
- atom_type: int32 [8, 2, 2, 768], P(('win', 'dx'), 'dy', 'dz'), parts along dimension 0, may hold values from 0 to 31
- perturbed: int32 [8, 2, 2, 768], P(('win', 'dx'), 'dy', 'dz'), parts along dimension 0, may hold values from 0 to 1
- leaving: int32 [8, 2, 2, 2, 16], P(('win', 'dx'), 'dy', 'dz'), parts along dimension 0, may hold values from 0 to 767, as said below
- neighbours: int32 [8, 2, 2, 6, 16], P(('win', 'dx'), 'dy', 'dz'), parts along dimension 0, may hold values from 0 to 161, as said below
- counts: int32 [8, 2, 2, 6], P(('win', 'dx'), 'dy', 'dz'), parts along dimension 0, may hold values from 1 to 16, as said below
- sigma_table: float32 [32], replicated, may hold values from 0.8 to 1.2
- depth_table: float32 [32], replicated, may hold values from 0.002 to 0.03
- charge_table: float32 [32], replicated, may hold values from -1 to 1
- domain_edge: float32 [3], replicated, may hold values from 1 to 1.12
- coupling: float32 [2], P('win'), parts along dimension 0, may hold values from 0.1 to 0.9
Outputs:
- forces: float32 [3, 8, 2, 2, 768], P(None, ('win', 'dx'), 'dy', 'dz'), parts along dimension 1
- energy: float32 [2], P('win'), parts along dimension 0
- dhdl: float32 [2], P('win'), parts along dimension 0
The draws below stay inside these ranges and needn't reach their ends.
There are 2 independent parts, one for each index of `win`. The reference program is written for one: setup_inputs(seed, part) draws one part's arguments, and reference() takes and returns one part's arrays. A program takes and returns all parts, laid end to end along the dimension named above; an argument that names none is the same for every part. Nothing has to cross between parts.
Inputs may be any that keep to these rules, and one draw needn't show every extreme that they name: `leaving`: each domain lists 2 * 16 distinct slots: the first 16 leave toward the next domain, the last 16 toward the previous one. `neighbours`: each list holds 16 distinct ghost block numbers; entries at or past the block's count are valid numbers and are not used. `counts`: some block lists exactly 16 blocks in every draw.
All inputs are finite; a program needn't handle non-finite values.
Results may differ from the reference program's by a relative error of at most 0.0003.
Values sent between devices are 32-bit elements; how exact they have to be, the bound alone decides.
A program may use at most 64 MiB of HBM per device.

```python
import math
import jax
import jax.numpy as jnp
from jax import lax

ATOMS_DEV = 768
NB = 16
MIG = 16
NTYPES = 32
NATOMS = 12288
N_DX = 4
N_DY = 2
N_DZ = 2


def draw_perturbed(key, part):
    shape = (N_DX, N_DY, N_DZ, ATOMS_DEV)
    position_x = jnp.arange(N_DX, dtype=jnp.int32)[:, None, None, None]
    threshold = 10 + 20 * position_x // max(N_DX - 1, 1)
    values = jax.random.randint(key, shape, 0, 100, dtype=jnp.int32)
    return (values < threshold).astype(jnp.int32)


def draw_leaving(key, part):
    shape = (N_DX, N_DY, N_DZ, ATOMS_DEV)
    scores = jax.random.randint(key, shape, 0, 2 ** 16, dtype=jnp.int32) * ATOMS_DEV + jnp.arange(ATOMS_DEV, dtype=jnp.int32)
    order = jnp.argsort(scores, axis=-1, stable=True).astype(jnp.int32)
    return order[..., :2 * MIG].reshape(N_DX, N_DY, N_DZ, 2, MIG)


def draw_neighbours(key, part):
    ghost_blocks = 27 * (ATOMS_DEV // 128)
    shape = (N_DX, N_DY, N_DZ, ATOMS_DEV // 128, ghost_blocks)
    scores = jax.random.randint(key, shape, 0, 2 ** 16, dtype=jnp.int32) * ghost_blocks + jnp.arange(ghost_blocks, dtype=jnp.int32)
    order = jnp.argsort(scores, axis=-1, stable=True).astype(jnp.int32)
    return order[..., :NB]


def draw_counts(key, part):
    shape = (N_DX, N_DY, N_DZ, ATOMS_DEV // 128)
    values = jax.random.randint(key, shape, 1, NB + 1, dtype=jnp.int32)
    return values.at[0, 0, 0, 0].set(NB)


def touch_ends(array, key, smallest, top_value):
    longest = array.shape.index(max(array.shape))
    spots = []
    for shift in (0, 1):
        where = [jax.random.randint(jax.random.fold_in(key, axis), (), 0, length) for axis, length in enumerate(array.shape)]
        where[longest] = (where[longest] + shift) % array.shape[longest]
        spots.append(tuple(where))
    return array.at[spots[0]].set(smallest).at[spots[1]].set(top_value)


def levels(own_key, extent, cuts, least, high):
    factor_of, own = 1.0, jax.random.fold_in(own_key, 6)
    for dim, parts in cuts:
        steps = jnp.exp(jax.random.uniform(jax.random.fold_in(own, dim), (parts,), jnp.float32, least / len(cuts), high / len(cuts)))
        factor_of = factor_of * jnp.repeat(steps, extent[dim] // parts).reshape([-1 if axis == dim else 1 for axis in range(len(extent))])
    return factor_of


def setup_inputs(seed: int = 0, part: int = 0) -> dict:
    seeds = jax.random.split(jax.random.key(seed), 12)
    part_splits = jax.random.split(jax.random.fold_in(seeds[11], part), 12)
    fraction = jnp.clip(1.0 * jax.random.uniform(part_splits[0], (3, N_DX, N_DY, N_DZ, ATOMS_DEV), jnp.float32) ** levels(part_splits[0], (3, N_DX, N_DY, N_DZ, ATOMS_DEV), ((1, 4), (2, 2), (3, 2)), -0.2, 0.2), 0.0, 1.0)
    atom_type = touch_ends(jax.random.randint(part_splits[1], (N_DX, N_DY, N_DZ, ATOMS_DEV), 0, NTYPES), jax.random.fold_in(part_splits[1], 1), 0, NTYPES - 1).astype(jnp.int32)
    perturbed = draw_perturbed(jax.random.fold_in(jax.random.fold_in(seeds[11], part), 71), part)
    leaving = draw_leaving(jax.random.fold_in(jax.random.fold_in(seeds[11], part), 71), part)
    neighbours = draw_neighbours(jax.random.fold_in(jax.random.fold_in(seeds[11], part), 71), part)
    counts = draw_counts(jax.random.fold_in(jax.random.fold_in(seeds[11], part), 71), part)
    sigma_table = jnp.clip(jnp.exp(jax.random.uniform(seeds[6], (NTYPES,), jnp.float32, math.log(0.8), math.log(1.2))), 0.8, 1.2)
    depth_table = jnp.clip(jnp.exp(jax.random.uniform(seeds[7], (NTYPES,), jnp.float32, math.log(0.002), math.log(0.03))), 0.002, 0.03)
    charge_table = jnp.clip(jax.random.uniform(seeds[8], (NTYPES,), jnp.float32, -1.0, 1.0), -1.0, 1.0)
    domain_edge = jnp.clip(jax.random.uniform(seeds[9], (3,), jnp.float32, 1.0, 1.12), 1.0, 1.12)
    coupling = jnp.clip(jax.random.uniform(part_splits[10], (1,), jnp.float32, 0.1, 0.9), 0.1, 0.9)
    return {"fraction": fraction, "atom_type": atom_type, "perturbed": perturbed, "leaving": leaving, "neighbours": neighbours, "counts": counts, "sigma_table": sigma_table, "depth_table": depth_table, "charge_table": charge_table, "domain_edge": domain_edge, "coupling": coupling}


soft_base = 0.3
soft_alpha = 0.5
charge_base = 0.3
charge_alpha = 0.5
coulomb = 0.1

def lookup(table_row, type_ids):
    onehot = type_ids[None, :] == jnp.arange(table_row.shape[0], dtype=jnp.int32)[:, None]
    return lax.optimization_barrier(jnp.sum(jnp.where(onehot, table_row[:, None], jnp.float32(0.0)), axis=0))

def pair_block(own_block, other_blocks, live_pairs, coupling_value):
    separation = own_block[0:3][None, :, :, None] - other_blocks[:, 0:3][:, :, None, :]
    radius_sq = lax.optimization_barrier(jnp.sum(separation * separation, axis=1))
    sigma_pair = 0.5 * (own_block[3][None, :, None] + other_blocks[:, 3][:, None, :])
    depth_pair = jnp.sqrt(own_block[4][None, :, None] * other_blocks[:, 4][:, None, :])
    charges = own_block[5][None, :, None] * other_blocks[:, 5][:, None, :]
    flagged = jnp.maximum(own_block[6][None, :, None], other_blocks[:, 6][:, None, :])
    scaled = coupling_value * flagged
    sigma_two = sigma_pair * sigma_pair
    sigma_six = sigma_two * sigma_two * sigma_two
    soft_six = sigma_six * (soft_base + soft_alpha * scaled) + radius_sq * radius_sq * radius_sq
    soft_two = charge_base + charge_alpha * scaled + radius_sq
    inverse_six = 1.0 / soft_six
    energy_lj = 4.0 * depth_pair * (sigma_six * sigma_six * inverse_six * inverse_six - sigma_six * inverse_six)
    grad_six = 4.0 * depth_pair * (sigma_six * inverse_six * inverse_six - 2.0 * sigma_six * sigma_six * inverse_six * inverse_six * inverse_six)
    energy_coul = coulomb * charges * lax.rsqrt(soft_two)
    grad_two = -0.5 * energy_coul / soft_two
    weight = 1.0 - scaled
    total_pair = energy_lj + energy_coul
    pair_energy = jnp.sum(weight * total_pair * live_pairs)
    pair_dhdl = jnp.sum(flagged * (-total_pair + weight * (grad_six * sigma_six * soft_alpha + grad_two * charge_alpha)) * live_pairs)
    force_scale = -weight * (6.0 * radius_sq * radius_sq * grad_six + 2.0 * grad_two) * live_pairs
    forces = lax.optimization_barrier(jnp.sum(force_scale[:, None] * separation, axis=(0, 3)))
    return (forces, pair_energy, pair_dhdl)

def block_terms(ghost_rows, listed_blocks, list_count, block_id, block_total, coupling_value):
    centre = 13 * block_total + block_id
    own_block = lax.dynamic_index_in_dim(ghost_rows, centre, 0, keepdims=False)
    other_blocks = jnp.take(ghost_rows, listed_blocks, axis=0)
    valid_slot = (jnp.arange(listed_blocks.shape[0], dtype=jnp.int32) < list_count).astype(jnp.float32)
    is_self = (listed_blocks == centre).astype(jnp.float32)[:, None, None] * jnp.eye(128, dtype=jnp.float32)[None]
    live_pairs = valid_slot[:, None, None] * (1.0 - is_self)
    return pair_block(own_block, other_blocks, live_pairs, coupling_value)

def reference(fraction, atom_type, perturbed, leaving, neighbours, counts, sigma_table, depth_table, charge_table, domain_edge, coupling):
    domains = N_DX * N_DY * N_DZ
    block_total = ATOMS_DEV // 128
    spacing = float(ATOMS_DEV) ** (1.0 / 3.0)
    type_ids = atom_type.reshape(-1)
    payload = jnp.concatenate([fraction.reshape(3, domains, ATOMS_DEV), lookup(sigma_table, type_ids).reshape(1, domains, ATOMS_DEV), lookup(depth_table, type_ids).reshape(1, domains, ATOMS_DEV), lookup(charge_table, type_ids).reshape(1, domains, ATOMS_DEV), perturbed.reshape(1, domains, ATOMS_DEV).astype(jnp.float32)], axis=0)
    leave_slots = leaving.reshape(domains, 2, MIG)
    upward = jnp.take_along_axis(payload, leave_slots[None, :, 0, :], axis=2)
    downward = jnp.take_along_axis(payload, leave_slots[None, :, 1, :], axis=2)
    shift_x = jnp.zeros((7, 1, 1), jnp.float32).at[0].set(1.0)
    from_below = jnp.roll(upward.reshape(7, N_DX, N_DY * N_DZ, MIG), 1, axis=1).reshape(7, domains, MIG) - shift_x
    from_above = jnp.roll(downward.reshape(7, N_DX, N_DY * N_DZ, MIG), -1, axis=1).reshape(7, domains, MIG) + shift_x

    def place(block_rows, down_slots, up_slots, lower_rows, upper_rows):
        return block_rows.at[:, down_slots].set(lower_rows).at[:, up_slots].set(upper_rows)
    moved = jax.vmap(place, in_axes=(1, 0, 0, 1, 1), out_axes=1)(payload, leave_slots[:, 1], leave_slots[:, 0], from_below, from_above)
    moved_grid = moved.reshape(7, N_DX, N_DY, N_DZ, ATOMS_DEV)
    list_flat = neighbours.reshape(domains, block_total, NB)
    count_flat = counts.reshape(domains, block_total)
    coupling_value = coupling[0]

    def one_domain(flat_id):
        index_x = flat_id // (N_DY * N_DZ)
        index_y = flat_id // N_DZ % N_DY
        index_z = flat_id % N_DZ
        pieces = []
        for step_x in range(3):
            for step_y in range(3):
                for step_z in range(3):
                    neighbour_rows = moved_grid[:, (index_x + step_x - 1) % N_DX, (index_y + step_y - 1) % N_DY, (index_z + step_z - 1) % N_DZ]
                    position = jnp.stack([(neighbour_rows[0] + jnp.float32(step_x - 1)) * domain_edge[0] * spacing, (neighbour_rows[1] + jnp.float32(step_y - 1)) * domain_edge[1] * spacing, (neighbour_rows[2] + jnp.float32(step_z - 1)) * domain_edge[2] * spacing], axis=0)
                    pieces.append(jnp.concatenate([position, neighbour_rows[3:]], axis=0))
        ghost_rows = jnp.stack(pieces, 0).reshape(27, 7, block_total, 128).transpose(0, 2, 1, 3).reshape(27 * block_total, 7, 128)
        listed = list_flat[flat_id]
        listed_count = count_flat[flat_id]

        def one_block(block_id):
            return block_terms(ghost_rows, listed[block_id], listed_count[block_id], block_id, block_total, coupling_value)
        forces, energies, dhdls = lax.map(one_block, jnp.arange(block_total, dtype=jnp.int32))
        return (forces.transpose(1, 0, 2).reshape(3, ATOMS_DEV), jnp.sum(energies), jnp.sum(dhdls))
    forces, energies, dhdls = lax.map(one_domain, jnp.arange(domains, dtype=jnp.int32))
    forces = forces.transpose(1, 0, 2).reshape(3, N_DX, N_DY, N_DZ, ATOMS_DEV)
    energy = (0.5 * jnp.sum(energies) / jnp.float32(NATOMS)).reshape(1)
    dhdl = (0.5 * jnp.sum(dhdls) / jnp.float32(NATOMS)).reshape(1)
    return (forces, energy, dhdl)
```

```python
import jax
import jax.numpy as jnp
from jax import lax
from jax.experimental import pallas as pl
from jax.experimental.pallas import tpu as pltpu
from jax.sharding import PartitionSpec as P

soft_base = 0.3
soft_alpha = 0.5
charge_base = 0.3
charge_alpha = 0.5
coulomb = 0.1
LANES = 128
MESH = pl.DeviceIdType.MESH
HIGHEST = lax.Precision.HIGHEST


def steps_of(count):
    return {1: (0,), 2: (0, 1)}.get(count, (-1, 0, 1))


def slot_step(step, count):
    if count == 1:
        return step * 0
    if count == 2:
        return step * step
    return step + 1


def thirds(value):
    high = value.astype(jnp.bfloat16).astype(jnp.float32)
    rest = value - high
    middle = rest.astype(jnp.bfloat16).astype(jnp.float32)
    return jnp.concatenate([high, middle, rest - middle], axis=0)


def joined(value):
    return value[0:8] + value[8:16] + value[16:24]


def step_kernel(
    sizes,
    *refs,
):
    inputs, refs = refs[:11], refs[11:]
    force_ref, tally_ref, *refs = refs
    staged, (load_sem, *refs) = refs[:11], refs[11:]
    (
        edge_ref,
        coupling_ref,
        sigma_ref,
        depth_ref,
        charge_ref,
        listed_ref,
        count_ref,
        fraction_ref,
        type_ref,
        flag_ref,
        leaving_ref,
    ) = staged
    (
        ghost_ref,
        outgoing,
        incoming,
        own_cols,
        force_acc,
        params,
        sums_ref,
        tile,
        gathered,
        mig_send,
        mig_recv,
        send_sem,
        recv_sem,
        sum_send,
        sum_recv,
    ) = refs
    nx, ny, nz = sizes
    atoms = fraction_ref.shape[-1]
    spacing = float(atoms) ** (1.0 / 3.0)
    me = (lax.axis_index("dx"), lax.axis_index("dy"), lax.axis_index("dz"))

    def device(step):
        return {
            name: lax.rem(place + by + count, count)
            for name, place, by, count in zip(("dx", "dy", "dz"), me, step, sizes)
        }

    offsets = [(a, b, c) for a in steps_of(nx) for b in steps_of(ny) for c in steps_of(nz)]
    others = [o for o in offsets if any(o)]

    def slot(o):
        return (
            slot_step(o[0], nx) * len(steps_of(ny)) + slot_step(o[1], ny)
        ) * len(steps_of(nz)) + slot_step(o[2], nz)

    barrier = pltpu.get_barrier_semaphore()
    total = nx * ny * nz
    my_id = (me[0] * ny + me[1]) * nz + me[2]

    def window_device(k):
        return {
            "dx": lax.div(k, ny * nz),
            "dy": lax.rem(lax.div(k, nz), ny),
            "dz": lax.rem(k, nz),
        }

    @pl.loop(1, total)
    def _(by):
        pl.semaphore_signal(
            barrier,
            inc=1,
            device_id=window_device(lax.rem(my_id + by, total)),
            device_id_type=MESH,
        )

    loads = [
        pltpu.make_async_copy(source, target, load_sem.at[k])
        for k, (source, target) in enumerate(zip(inputs, staged))
    ]
    for load in loads:
        load.start()
    for load in loads:
        load.wait()

    own = ghost_ref.at[slot((0, 0, 0))]
    edge = [edge_ref[k] * spacing for k in range(3)]
    rows = [fraction_ref[k, 0, 0] * edge[k] for k in range(3)]
    rows += [type_ref[0, 0].astype(jnp.float32), flag_ref[0, 0].astype(jnp.float32)]
    payload = jnp.concatenate(rows + [jnp.zeros((3, atoms), jnp.float32)], axis=0)
    leave = leaving_ref[0, 0, 0]
    mig = leave.shape[1]
    slots_in = jnp.concatenate([leave[0:1], leave[1:2]], axis=1)
    slots_out = jnp.concatenate([leave[1:2], leave[0:1]], axis=1)
    place = lax.broadcasted_iota(jnp.int32, (atoms, 2 * mig), 0)
    hot_in = (place == slots_in).astype(jnp.float32).astype(jnp.bfloat16)
    hot_out = (place == slots_out).astype(jnp.float32).astype(jnp.bfloat16)
    lane = lax.broadcasted_iota(jnp.int32, (8, 2 * mig), 1)
    first = lax.broadcasted_iota(jnp.int32, (8, 2 * mig), 0) == 0
    shift = jnp.where(first, jnp.where(lane < mig, edge[0], -edge[0]), 0.0)
    leavers = joined(
        jnp.dot(thirds(payload).astype(jnp.bfloat16), hot_out, preferred_element_type=jnp.float32)
    )
    outgoing[...] = leavers + shift

    def spread(value):
        return lax.dot_general(
            value.astype(jnp.bfloat16),
            hot_in,
            (((1,), (1,)), ((), ())),
            preferred_element_type=jnp.float32,
        )

    gone = spread(jnp.ones((8, 2 * mig), jnp.float32))

    pl.semaphore_wait(barrier, total - 1)
    moves = []
    for side, by in ((0, 1), (1, -1)):
        move = pltpu.make_async_remote_copy(
            src_ref=outgoing,
            dst_ref=incoming.at[side],
            send_sem=mig_send.at[side],
            recv_sem=mig_recv.at[side],
            device_id=device((by, 0, 0)),
            device_id_type=MESH,
        )
        move.start()
        moves.append(move)
    for move in moves:
        move.wait()
    merged = jnp.where(lane < mig, incoming[1], incoming[0])
    moved = jnp.where(gone > 0.5, joined(spread(thirds(merged))), payload)
    for r in range(5):
        own[r] = moved[r : r + 1]
    copies = []
    for k, o in enumerate(sorted(others, key=lambda o: -sum(map(abs, o)))):
        copy = pltpu.make_async_remote_copy(
            src_ref=own,
            dst_ref=ghost_ref.at[slot(o)],
            send_sem=send_sem.at[k],
            recv_sem=recv_sem.at[k],
            device_id=device(tuple(-x for x in o)),
            device_id_type=MESH,
        )
        copy.start()
        copies.append((copy, slot(o)))

    blocks = atoms // LANES
    lam = coupling_ref[0]
    own_slot = slot((0, 0, 0))
    ones = jnp.ones((8, LANES), jnp.bfloat16)
    for k in range(3):
        sums_ref[k] = jnp.zeros((8, LANES), jnp.float32)

    ahead = lax.broadcasted_iota(jnp.int32, (8, LANES), 1) - lax.broadcasted_iota(
        jnp.int32, (8, LANES), 0
    )
    lane = lax.broadcasted_iota(jnp.int32, (1, LANES), 1)
    tables = [jnp.zeros((1, LANES), jnp.float32)] * 3
    for k in range(sigma_ref.shape[0]):
        hit = lane == k
        tables = [
            jnp.where(hit, ref[k], table)
            for ref, table in zip((sigma_ref, depth_ref, charge_ref), tables)
        ]
    table = jnp.concatenate(
        [tables[0] * 0.5, jnp.sqrt(tables[1]) * 2.0, tables[2]] + [tables[2] * 0.0] * 5, axis=0
    )
    kinds = sigma_ref.shape[0]
    table_parts = thirds(table[:, :kinds]).astype(jnp.bfloat16)
    kind_row = lax.broadcasted_iota(jnp.int32, (kinds, atoms), 0).astype(jnp.float32)

    def look_up(place):
        onehot = (kind_row == ghost_ref[place, 3]).astype(jnp.float32).astype(jnp.bfloat16)
        found = joined(jnp.dot(table_parts, onehot, preferred_element_type=jnp.float32))
        rows = [ghost_ref[place, r] for r in range(3)]
        rows += [found[0:3], ghost_ref[place, 4], found[3:4]]
        whole = jnp.concatenate(rows, axis=0)
        for q in range(blocks):
            params[place * blocks + q] = whole[:, q * LANES : (q + 1) * LANES]

    look_up(own_slot)
    picks = (
        lax.broadcasted_iota(jnp.int32, (24, 7 * LANES), 0) % 8
        == lax.broadcasted_iota(jnp.int32, (24, 7 * LANES), 1) // LANES
    ).astype(jnp.float32).astype(jnp.bfloat16)
    for q in range(blocks):
        cols = thirds(params[own_slot * blocks + q]).T.astype(jnp.bfloat16)
        wide = jnp.dot(cols, picks, preferred_element_type=jnp.float32)
        for r in range(7):
            col = wide[:, r * LANES : (r + 1) * LANES]
            own_cols[q, r] = col * coulomb if r == 5 else col
    for q in range(blocks):
        for k in range(3):
            force_acc[q, k] = jnp.zeros((LANES, LANES), jnp.float32)

    for copy, place in copies:
        copy.wait()
        look_up(place)

    @pl.loop(0, blocks)
    def _(q):
        def entry(e):
            listed = listed_ref[q, 0, e]
            left = jnp.minimum(jnp.maximum(count_ref[0, 0, 0, q] - e, 0), 1)
            used = left.astype(jnp.float32)
            apart = jnp.abs(listed - (13 * blocks + q))
            self_lane = jnp.minimum(apart, 1) * (2 * LANES)
            image = lax.div(listed, blocks)
            a = lax.div(image, 9) - 1
            b = lax.rem(lax.div(image, 3), 3) - 1
            c = lax.rem(image, 3) - 1
            where_from = (
                slot_step(a, nx) * len(steps_of(ny)) + slot_step(b, ny)
            ) * len(steps_of(nz)) + slot_step(c, nz)
            other = params[where_from * blocks + lax.rem(listed, blocks)]
            rows = []
            for r in range(7):
                row = other[r : r + 1]
                if r < 3:
                    row = row + (a, b, c)[r].astype(jnp.float32) * edge[r]
                if 4 <= r < 6:
                    row = row * used
                rows.append(jnp.broadcast_to(row, (8, LANES)))
            xj, yj, zj, hj, ej, qj, pj = rows

            tot = jnp.zeros((8, LANES), jnp.float32)
            tot_p = jnp.zeros((8, LANES), jnp.float32)
            tot_k = jnp.zeros((8, LANES), jnp.float32)
            for g in range(LANES // 8):
                at = pl.ds(g * 8, 8)
                dx = own_cols[q, 0, at] - xj
                dy = own_cols[q, 1, at] - yj
                dz = own_cols[q, 2, at] - zj
                r2 = dx * dx + dy * dy + dz * dz
                sig = own_cols[q, 3, at] + hj
                s2 = sig * sig
                s6 = s2 * s2 * s2
                eps4 = own_cols[q, 4, at] * ej
                qq = own_cols[q, 5, at] * qj
                diag = ahead == self_lane + g * 8
                eps4 = jnp.where(diag, 0.0, eps4)
                qq = jnp.where(diag, 0.0, qq)
                p = jnp.maximum(own_cols[q, 6, at], pj)
                soft = soft_base + (soft_alpha * lam) * p
                weight = 1.0 - lam * p
                r4 = r2 * r2
                soft6 = s6 * soft + r4 * r2
                inv = 1.0 / soft6
                u = lax.rsqrt(soft + r2)
                ec = qq * u
                half = (0.5 * ec) * (u * u)
                t = s6 * inv
                et = eps4 * t
                tm = t - 1.0
                v = et * tm + ec
                m = et * (t + tm)
                kk = m * t + half
                fs = weight * (3.0 * (m * (r4 * inv)) + half)
                tot = tot + v
                tot_p = tot_p + p * v
                tot_k = tot_k + p * kk
                force_acc[q, 0, at] += fs * dx
                force_acc[q, 1, at] += fs * dy
                force_acc[q, 2, at] += fs * dz
            sums_ref[0] += tot
            sums_ref[1] += tot_p
            sums_ref[2] += tot_k

        width = listed_ref.shape[-1]
        unroll = 4 if width % 4 == 0 else 1

        @pl.loop(0, width // unroll)
        def _(step):
            for k in range(unroll):
                entry(step * unroll + k)

    folded = [jnp.sum(sums_ref[k], axis=0, keepdims=True) for k in range(3)]
    folded.append(jnp.zeros((5, LANES), jnp.float32))
    mine = jnp.concatenate(folded, axis=0)
    tile[...] = mine
    gathered[my_id] = mine

    def share(by):
        return pltpu.make_async_remote_copy(
            src_ref=tile,
            dst_ref=gathered.at[my_id],
            send_sem=sum_send.at[by],
            recv_sem=sum_recv.at[by],
            device_id=window_device(lax.rem(my_id + by, total)),
            device_id_type=MESH,
        )

    @pl.loop(1, total)
    def _(by):
        share(by).start()

    for q in range(blocks):
        for k in range(3):
            whole = force_acc[q, k]
            high = whole.astype(jnp.bfloat16)
            low = (whole - high.astype(jnp.float32)).astype(jnp.bfloat16)
            reduced = sum(
                lax.dot_general(
                    ones, part, (((1,), (1,)), ((), ())), preferred_element_type=jnp.float32
                )
                for part in (high, low)
            )
            force_ref[k, 0, 0, :, q * LANES : (q + 1) * LANES] = 2.0 * reduced[0:1]

    @pl.loop(1, total)
    def _(by):
        share(by).wait()

    summed = jnp.sum(gathered[...], axis=0)
    parts = [jnp.sum(summed[k : k + 1]) for k in range(3)]
    scale = 0.5 / float(atoms * total)
    rows = lax.broadcasted_iota(jnp.int32, (8, LANES), 0)
    energy = scale * (parts[0] - lam * parts[1])
    dhdl = -scale * (parts[1] + (0.5 * (1.0 - lam)) * parts[2])
    tally_ref[...] = jnp.where(rows == 0, energy, dhdl)


def hand_over(force_in, tally_in, force_ref, energy_ref, dhdl_ref, sem):
    copy = pltpu.make_async_copy(force_in, force_ref, sem)
    copy.start()
    energy_ref[0] = tally_in[0, 0]
    dhdl_ref[0] = tally_in[1, 0]
    copy.wait()


def on_device(sizes, fraction, atom_type, perturbed, leaving, neighbours, counts,
              sigma_table, depth_table, charge_table, domain_edge, coupling):
    nx, ny, nz = sizes
    atoms = fraction.shape[-1]
    mig = leaving.shape[-1]
    slots = len(steps_of(nx)) * len(steps_of(ny)) * len(steps_of(nz))
    smem = pl.BlockSpec(memory_space=pltpu.SMEM)
    vmem = pl.BlockSpec(memory_space=pltpu.VMEM)
    f32 = jnp.float32

    def bound(kernel, *values):
        return lambda *refs: kernel(*values, *refs)

    blocks = atoms // LANES
    total = nx * ny * nz
    dma = pltpu.SemaphoreType.DMA
    arrays = (
        domain_edge,
        coupling,
        sigma_table,
        depth_table,
        charge_table,
        neighbours.reshape(blocks, 1, -1),
        counts,
        fraction,
        atom_type,
        perturbed,
        leaving,
    )
    forces, tally = pl.pallas_call(
        bound(step_kernel, sizes),
        name="step",
        out_shape=(pltpu.VMEM(fraction.shape, f32), pltpu.VMEM((8, LANES), f32)),
        in_specs=[pl.BlockSpec(memory_space=pl.ANY)] * 11,
        out_specs=(vmem, vmem),
        scratch_shapes=[
            *(pltpu.SMEM(x.shape, x.dtype) for x in arrays[:7]),
            *(pltpu.VMEM(x.shape, x.dtype) for x in arrays[7:]),
            dma((11,)),
            pltpu.VMEM((slots, 5, 1, atoms), f32),
            pltpu.VMEM((8, 2 * mig), f32),
            pltpu.VMEM((2, 8, 2 * mig), f32),
            pltpu.VMEM((blocks, 7, LANES, LANES), f32),
            pltpu.VMEM((blocks, 3, LANES, LANES), f32),
            pltpu.VMEM((slots * blocks, 8, LANES), f32),
            pltpu.VMEM((3, 8, LANES), f32),
            pltpu.VMEM((8, LANES), f32),
            pltpu.VMEM((total, 8, LANES), f32),
            dma((2,)),
            dma((2,)),
            dma((slots,)),
            dma((slots,)),
            dma((total,)),
            dma((total,)),
        ],
        compiler_params=pltpu.CompilerParams(collective_id=0, has_side_effects=True),
    )(*arrays)
    return pl.pallas_call(
        hand_over,
        name="hand_over",
        out_shape=(
            jax.ShapeDtypeStruct(fraction.shape, f32),
            jax.ShapeDtypeStruct((1,), f32),
            jax.ShapeDtypeStruct((1,), f32),
        ),
        in_specs=[vmem, vmem],
        out_specs=(pl.BlockSpec(memory_space=pl.ANY), smem, smem),
        scratch_shapes=[pltpu.SemaphoreType.DMA],
    )(pltpu.with_memory_space_constraint(forces, pltpu.VMEM), pltpu.with_memory_space_constraint(tally, pltpu.VMEM))


def solution(mesh):
    sizes = (mesh.shape["dx"], mesh.shape["dy"], mesh.shape["dz"])
    return jax.shard_map(
        lambda *arrays: on_device(sizes, *arrays),
        mesh=mesh,
        in_specs=(
            P(None, ("win", "dx"), "dy", "dz", None),
            P(("win", "dx"), "dy", "dz", None),
            P(("win", "dx"), "dy", "dz", None),
            P(("win", "dx"), "dy", "dz", None, None),
            P(("win", "dx"), "dy", "dz", None, None),
            P(("win", "dx"), "dy", "dz", None),
            P(),
            P(),
            P(),
            P(),
            P("win"),
        ),
        out_specs=(P(None, ("win", "dx"), "dy", "dz", None), P("win"), P("win")),
        check_vma=False,
    )
```

```python
import jax
import jax.numpy as jnp
from jax import lax
from jax.experimental import pallas as pl
from jax.experimental.pallas import tpu as pltpu
from jax.sharding import PartitionSpec as P

soft_base = 0.3
soft_alpha = 0.5
charge_base = 0.3
charge_alpha = 0.5
coulomb = 0.1
LANES = 128
MESH = pl.DeviceIdType.MESH
ROWS = 5
FORMS = 6


def steps_of(count):
    return {1: (0,), 2: (0, 1)}.get(count, (-1, 0, 1))


def slot_step(step, count):
    if count == 1:
        return step * 0
    if count == 2:
        return step * step
    return step + 1


def split(value):
    high = value.astype(jnp.bfloat16).astype(jnp.float32)
    rest = value - high
    middle = rest.astype(jnp.bfloat16).astype(jnp.float32)
    return high, middle, rest - middle


def thirds(value):
    return jnp.concatenate(split(value), axis=0)


def onehot(hits):
    return hits.astype(jnp.float32).astype(jnp.bfloat16)


def joined(value):
    return value[0:8] + value[8:16] + value[16:24]


def step_kernel(
    sizes,
    *refs,
):
    inputs, refs = refs[:11], refs[11:]
    force_ref, tally_ref, *refs = refs
    staged, (load_sem, *refs) = refs[:11], refs[11:]
    (
        edge_ref,
        coupling_ref,
        listed_ref,
        count_ref,
        sigma_ref,
        depth_ref,
        charge_ref,
        fraction_ref,
        type_ref,
        flag_ref,
        leaving_ref,
    ) = staged
    (
        ghost_ref,
        outgoing,
        incoming,
        own_cols,
        force_acc,
        table_ref,
        lhs_ref,
        self_ref,
        forms_a,
        forms_b,
        sums_ref,
        tile,
        gathered,
        mig_send,
        mig_recv,
        send_sem,
        recv_sem,
        sum_send,
        sum_recv,
    ) = refs
    nx, ny, nz = sizes
    atoms = fraction_ref.shape[-1]
    blocks = atoms // LANES
    width = listed_ref.shape[-1]
    kinds = sigma_ref.shape[-1]
    spacing = float(atoms) ** (1.0 / 3.0)
    me = (lax.axis_index("dx"), lax.axis_index("dy"), lax.axis_index("dz"))

    def device(step):
        return {
            name: lax.rem(place + by + count, count)
            for name, place, by, count in zip(("dx", "dy", "dz"), me, step, sizes)
        }

    offsets = [(a, b, c) for a in steps_of(nx) for b in steps_of(ny) for c in steps_of(nz)]
    others = [o for o in offsets if any(o)]

    def slot(o):
        return (
            slot_step(o[0], nx) * len(steps_of(ny)) + slot_step(o[1], ny)
        ) * len(steps_of(nz)) + slot_step(o[2], nz)

    barrier = pltpu.get_barrier_semaphore()
    total = nx * ny * nz
    my_id = (me[0] * ny + me[1]) * nz + me[2]

    def window_device(k):
        return {
            "dx": lax.div(k, ny * nz),
            "dy": lax.rem(lax.div(k, nz), ny),
            "dz": lax.rem(k, nz),
        }

    @pl.loop(1, total)
    def _(by):
        pl.semaphore_signal(
            barrier,
            inc=1,
            device_id=window_device(lax.rem(my_id + by, total)),
            device_id_type=MESH,
        )

    loads = [
        pltpu.make_async_copy(source, target, load_sem.at[k])
        for k, (source, target) in enumerate(zip(inputs, staged))
    ]
    for load in loads:
        load.start()
    for load in loads:
        load.wait()

    own = ghost_ref.at[slot((0, 0, 0))]
    edge = [edge_ref[k] * (spacing * 3.0**-0.5) for k in range(3)]
    rows = [(fraction_ref[k, 0, 0] - 0.5) * edge[k] for k in range(3)]
    rows += [type_ref[0, 0].astype(jnp.float32), flag_ref[0, 0].astype(jnp.float32)]
    payload = jnp.concatenate(rows + [jnp.zeros((3, atoms), jnp.float32)], axis=0)
    leave = leaving_ref[0, 0, 0]
    mig = leave.shape[1]
    slots_in = jnp.concatenate([leave[0:1], leave[1:2]], axis=1)
    slots_out = jnp.concatenate([leave[1:2], leave[0:1]], axis=1)
    place = lax.broadcasted_iota(jnp.int32, (atoms, 2 * mig), 0)
    hot_in = (place == slots_in).astype(jnp.float32).astype(jnp.bfloat16)
    hot_out = (place == slots_out).astype(jnp.float32).astype(jnp.bfloat16)
    lane = lax.broadcasted_iota(jnp.int32, (8, 2 * mig), 1)
    first = lax.broadcasted_iota(jnp.int32, (8, 2 * mig), 0) == 0
    shift = jnp.where(first, jnp.where(lane < mig, edge[0], -edge[0]), 0.0)
    leavers = joined(
        jnp.dot(thirds(payload).astype(jnp.bfloat16), hot_out, preferred_element_type=jnp.float32)
    )
    outgoing[...] = leavers + shift

    def spread(value):
        return lax.dot_general(
            value.astype(jnp.bfloat16),
            hot_in,
            (((1,), (1,)), ((), ())),
            preferred_element_type=jnp.float32,
        )

    gone = spread(jnp.ones((8, 2 * mig), jnp.float32))

    pl.semaphore_wait(barrier, total - 1)
    moves = []
    for side, by in ((0, 1), (1, -1)):
        move = pltpu.make_async_remote_copy(
            src_ref=outgoing,
            dst_ref=incoming.at[side],
            send_sem=mig_send.at[side],
            recv_sem=mig_recv.at[side],
            device_id=device((by, 0, 0)),
            device_id_type=MESH,
        )
        move.start()
        moves.append(move)
    for move in moves:
        move.wait()
    merged = jnp.where(lane < mig, incoming[1], incoming[0])
    moved = jnp.where(gone > 0.5, joined(spread(thirds(merged))), payload)
    for q in range(blocks):
        for r in range(ROWS):
            own[q, r] = moved[r : r + 1, q * LANES : (q + 1) * LANES]
    copies = []
    for k, o in enumerate(sorted(others, key=lambda o: -sum(map(abs, o)))):
        copy = pltpu.make_async_remote_copy(
            src_ref=own,
            dst_ref=ghost_ref.at[slot(o)],
            send_sem=send_sem.at[k],
            recv_sem=recv_sem.at[k],
            device_id=device(tuple(-x for x in o)),
            device_id_type=MESH,
        )
        copy.start()
        copies.append((copy, slot(o)))

    lam = coupling_ref[0]
    own_slot = slot((0, 0, 0))
    ones = jnp.ones((8, LANES), jnp.bfloat16)
    for k in range(2):
        sums_ref[k] = jnp.zeros((8, LANES), jnp.float32)

    pairs = 2 * kinds
    flat = lax.broadcasted_iota(jnp.int32, (1, LANES), 1)

    def per_kind(ref):
        row = ref[...]
        return jnp.concatenate([row] * (LANES // kinds), axis=1)

    halved = per_kind(sigma_ref) * 0.5
    depth = jnp.sqrt(per_kind(depth_ref)) * 2.0
    charge = per_kind(charge_ref)
    flag = jnp.where(lax.rem(flat, pairs) < kinds, 0.0, 1.0)
    stack = jnp.concatenate(
        [halved, depth, charge, flag, jnp.zeros((4, LANES), jnp.float32)], axis=0
    ).T

    def column(k):
        return jnp.broadcast_to(stack[:pairs, k : k + 1], (pairs, LANES))

    six = column(0) + halved
    six = six * six
    six = six * six * six * (1.0 / 27.0)
    either = jnp.maximum(column(3), flag)
    soft = soft_base + (soft_alpha * lam) * either
    weight = 1.0 - lam * either
    root2 = 2.0**0.5
    tables = [
        2.0 * soft,
        six,
        six * soft,
        column(1) * depth * weight,
        (column(2) * (coulomb * root2)) * charge * weight,
    ]
    low_half = lax.broadcasted_iota(jnp.int32, (pairs, LANES), 1) < pairs
    for f, whole in enumerate(tables):
        high, middle, low = split(whole)
        for half, part in enumerate(
            (jnp.where(low_half, high, middle), jnp.where(low_half, low, 0.0))
        ):
            at = (2 * f + half) * LANES
            table_ref[:, at : at + LANES] = jnp.concatenate(
                [part, jnp.zeros((LANES - pairs, LANES), jnp.float32)], axis=0
            ).astype(jnp.bfloat16)

    scaled = 2.0 / (1.0 - lam)
    soft = soft_base + (soft_alpha * lam) * flag
    weight = 1.0 - lam * flag
    root = lax.rsqrt(2.0 * soft)
    ratio = 1.0 / soft
    electric = (coulomb * root2) * charge * charge * weight * root
    strength = depth * depth * weight * ratio
    alone = strength * (ratio - 1.0) + electric
    slope = strength * (ratio + (ratio - 1.0)) * ratio + electric * (root * root)
    both = jnp.concatenate(
        [alone, flag * (scaled * alone + slope), jnp.zeros((6, LANES), jnp.float32)], axis=0
    )
    self_parts = thirds(both[:, :pairs]).astype(jnp.bfloat16)

    kind_rows = lax.broadcasted_iota(jnp.int32, (pairs, LANES), 0).astype(jnp.float32)
    kind_lane = lax.broadcasted_iota(jnp.int32, (LANES, LANES), 1).astype(jnp.float32)
    deep = lax.broadcasted_iota(jnp.int32, (8, LANES), 0)
    unit3 = jnp.where(deep == 3, 1.0, 0.0)
    picks = onehot(
        lax.broadcasted_iota(jnp.int32, (24, ROWS * LANES), 0) % 8
        == lax.broadcasted_iota(jnp.int32, (24, ROWS * LANES), 1) // LANES
    )

    def kind_of(place, block):
        return ghost_ref[place, block, 3] + float(kinds) * ghost_ref[place, block, 4]

    @pl.loop(0, blocks)
    def _(q):
        kind = kind_of(own_slot, q)
        xyz = [ghost_ref[own_slot, q, r] for r in range(3)]
        blank = jnp.zeros((1, LANES), jnp.float32)
        rows = jnp.concatenate(
            xyz + [ghost_ref[own_slot, q, 4], kind, blank, blank, blank], axis=0
        )
        wide = jnp.dot(
            thirds(rows).T.astype(jnp.bfloat16), picks, preferred_element_type=jnp.float32
        )
        for r in range(4):
            own_cols[q, r] = wide[:, r * LANES : (r + 1) * LANES]
        norm = xyz[0] * xyz[0] + xyz[1] * xyz[1] + xyz[2] * xyz[2]
        base = jnp.concatenate(
            [x * -2.0 for x in xyz] + [blank, norm, blank, blank, blank], axis=0
        )
        geo = []
        for factor in (1.0, 6.0):
            high, middle, low = split(base * factor)
            unit = unit3 * factor
            groups = [high + unit, middle, low, high + unit, middle, high + unit]
            above = jnp.zeros((pairs, LANES), jnp.float32)
            below = jnp.zeros((LANES - pairs - 48, LANES), jnp.float32)
            geo.append(jnp.concatenate([above] + groups + [below], axis=0).T)
        hot = onehot(wide[:, 4 * LANES : 5 * LANES] == kind_lane)
        looked = jnp.dot(hot, table_ref[...], preferred_element_type=jnp.float32)
        lhs_ref[q, 0:LANES, 0:LANES] = jnp.zeros((LANES, LANES), jnp.bfloat16)
        lhs_ref[q, 0:LANES, LANES : 2 * LANES] = geo[0].astype(jnp.bfloat16)
        for f in range(FORMS - 1):
            left = looked[:, 2 * f * LANES : (2 * f + 1) * LANES]
            right = looked[:, (2 * f + 1) * LANES : (2 * f + 2) * LANES]
            if f == 0:
                right = right + geo[1]
            at = slice((f + 1) * LANES, (f + 2) * LANES)
            lhs_ref[q, at, 0:LANES] = left.astype(jnp.bfloat16)
            lhs_ref[q, at, LANES : 2 * LANES] = right.astype(jnp.bfloat16)
        mine = joined(
            jnp.dot(self_parts, onehot(kind_rows == kind), preferred_element_type=jnp.float32)
        )
        for k in range(2):
            self_ref[q, k] = jnp.where(deep == 0, mine[k : k + 1], 0.0)
        for k in range(3):
            force_acc[q, k] = jnp.zeros((LANES, LANES), jnp.float32)

    for copy, place in copies:
        copy.wait()

    def entry(q, e):
        listed = listed_ref[q, 0, e]
        left = jnp.minimum(jnp.maximum(count_ref[0, 0, 0, q] - e, 0), 1)
        apart = jnp.abs(listed - (13 * blocks + q))
        image = lax.div(listed, blocks)
        step = (
            lax.div(image, 9) - 1,
            lax.rem(lax.div(image, 3), 3) - 1,
            lax.rem(image, 3) - 1,
        )
        where_from = (
            slot_step(step[0], nx) * len(steps_of(ny)) + slot_step(step[1], ny)
        ) * len(steps_of(nz)) + slot_step(step[2], nz)
        block = lax.rem(listed, blocks)
        away = (1 - left).astype(jnp.float32) * 1024.0
        by = [step[k].astype(jnp.float32) * edge[k] for k in range(3)]
        by[0] = by[0] + away
        xyz = [ghost_ref[where_from, block, r] + by[r] for r in range(3)]
        itself = ((1 - jnp.minimum(apart, 1)) * left).astype(jnp.float32)
        return where_from, block, xyz, left, itself

    def features(q, e):
        place, block, xyz, left, _ = entry(q, e)
        norm = xyz[0] * xyz[0] + xyz[1] * xyz[1] + xyz[2] * xyz[2]
        blank = jnp.zeros((1, LANES), jnp.float32)
        rows = jnp.concatenate(xyz + [norm, blank + 1.0, blank, blank, blank], axis=0)
        high, middle, low = split(rows)
        kind = kind_of(place, block) - (1 - left).astype(jnp.float32) * float(2 * pairs)
        hot = onehot(kind_rows == kind)
        near = jnp.concatenate([high, high, high, middle, middle, low], axis=0)
        near = jnp.concatenate(
            [near, jnp.zeros((2 * LANES - 3 * pairs - 48, LANES), jnp.float32)], axis=0
        ).astype(jnp.bfloat16)
        return jnp.concatenate([hot, hot, hot, near], axis=0)

    per_block = width // 2

    def produce(t, forms):
        q = lax.div(t, per_block)
        e = 2 * lax.rem(t, per_block)
        rhs = jnp.concatenate([features(q, e), features(q, e + 1)], axis=1)
        forms[...] = jnp.dot(lhs_ref[q], rhs, preferred_element_type=jnp.float32)

    def consume(t, forms):
        q = lax.div(t, per_block)
        e = 2 * lax.rem(t, per_block)
        others = []
        tot = jnp.zeros((8, LANES), jnp.float32)
        tot_p = jnp.zeros((8, LANES), jnp.float32)
        for k in range(2):
            place, block, xyz, _, itself = entry(q, e + k)
            others.append(
                [
                    jnp.broadcast_to(row, (8, LANES))
                    for row in xyz + [ghost_ref[place, block, 4]]
                ]
            )
            tot = tot - itself * self_ref[q, 0]
            tot_p = tot_p - itself * self_ref[q, 1]
        for g in range(LANES // 8):
            at = pl.ds(g * 8, 8)
            xi, yi, zi, pi = (own_cols[q, r, at] for r in range(4))
            fx = fy = fz = None
            for k, (xj, yj, zj, pj) in enumerate(others):
                r2, s2, s6, soft6, eps, qq = (
                    forms[f * LANES + g * 8 : f * LANES + g * 8 + 8, k * LANES : (k + 1) * LANES]
                    for f in range(FORMS)
                )
                r4 = r2 * r2
                inv = 1.0 / (soft6 + r4 * r2)
                u = lax.rsqrt(s2)
                ec = qq * u
                half = ec * (u * u)
                t6 = s6 * inv
                et = eps * t6
                tm = t6 - 1.0
                v = et * tm + ec
                m = et * (t6 + tm)
                kk = m * t6 + half
                fs = m * (r4 * inv) + half
                tot = tot + v
                tot_p = tot_p + jnp.maximum(pi, pj) * (scaled * v + kk)
                gx, gy, gz = fs * (xi - xj), fs * (yi - yj), fs * (zi - zj)
                fx, fy, fz = (gx, gy, gz) if fx is None else (fx + gx, fy + gy, fz + gz)
            force_acc[q, 0, at] += fx
            force_acc[q, 1, at] += fy
            force_acc[q, 2, at] += fz
        sums_ref[0] += tot
        sums_ref[1] += tot_p

    steps = blocks * per_block
    produce(0, forms_a)

    @pl.loop(0, steps // 2)
    def _(s):
        produce(2 * s + 1, forms_b)
        consume(2 * s, forms_a)
        produce(jnp.minimum(2 * s + 2, steps - 1), forms_a)
        consume(2 * s + 1, forms_b)

    folded = [jnp.sum(sums_ref[k], axis=0, keepdims=True) for k in range(2)]
    folded.append(jnp.zeros((6, LANES), jnp.float32))
    mine = jnp.concatenate(folded, axis=0)
    tile[...] = mine
    gathered[my_id] = mine

    def share(by):
        return pltpu.make_async_remote_copy(
            src_ref=tile,
            dst_ref=gathered.at[my_id],
            send_sem=sum_send.at[by],
            recv_sem=sum_recv.at[by],
            device_id=window_device(lax.rem(my_id + by, total)),
            device_id_type=MESH,
        )

    @pl.loop(1, total)
    def _(by):
        share(by).start()

    for q in range(blocks):
        for k in range(3):
            whole = force_acc[q, k]
            high = whole.astype(jnp.bfloat16)
            low = (whole - high.astype(jnp.float32)).astype(jnp.bfloat16)
            reduced = sum(
                lax.dot_general(
                    ones, part, (((1,), (1,)), ((), ())), preferred_element_type=jnp.float32
                )
                for part in (high, low)
            )
            force_ref[k, 0, 0, :, q * LANES : (q + 1) * LANES] = (2.0 * 3.0**0.5) * reduced[0:1]

    @pl.loop(1, total)
    def _(by):
        share(by).wait()

    summed = jnp.sum(gathered[...], axis=0)
    parts = [jnp.sum(summed[k : k + 1]) for k in range(2)]
    scale = 0.5 / float(atoms * total)
    rows = lax.broadcasted_iota(jnp.int32, (8, LANES), 0)
    energy = scale * parts[0]
    dhdl = (-0.5 * scale) * parts[1]
    tally_ref[...] = jnp.where(rows == 0, energy, dhdl)


def hand_over(force_in, tally_in, force_ref, energy_ref, dhdl_ref, sem):
    copy = pltpu.make_async_copy(force_in, force_ref, sem)
    copy.start()
    energy_ref[0] = tally_in[0, 0]
    dhdl_ref[0] = tally_in[1, 0]
    copy.wait()


def on_device(sizes, fraction, atom_type, perturbed, leaving, neighbours, counts,
              sigma_table, depth_table, charge_table, domain_edge, coupling):
    nx, ny, nz = sizes
    atoms = fraction.shape[-1]
    mig = leaving.shape[-1]
    slots = len(steps_of(nx)) * len(steps_of(ny)) * len(steps_of(nz))
    smem = pl.BlockSpec(memory_space=pltpu.SMEM)
    vmem = pl.BlockSpec(memory_space=pltpu.VMEM)
    f32 = jnp.float32

    def bound(kernel, *values):
        return lambda *refs: kernel(*values, *refs)

    blocks = atoms // LANES
    total = nx * ny * nz
    dma = pltpu.SemaphoreType.DMA
    arrays = (
        domain_edge,
        coupling,
        neighbours.reshape(blocks, 1, -1),
        counts,
        *(table.reshape(1, -1) for table in (sigma_table, depth_table, charge_table)),
        fraction,
        atom_type,
        perturbed,
        leaving,
    )
    forces, tally = pl.pallas_call(
        bound(step_kernel, sizes),
        name="step",
        out_shape=(pltpu.VMEM(fraction.shape, f32), pltpu.VMEM((8, LANES), f32)),
        in_specs=[pl.BlockSpec(memory_space=pl.ANY)] * 11,
        out_specs=(vmem, vmem),
        scratch_shapes=[
            *(pltpu.SMEM(x.shape, x.dtype) for x in arrays[:4]),
            *(pltpu.VMEM(x.shape, x.dtype) for x in arrays[4:]),
            dma((11,)),
            pltpu.VMEM((slots, blocks, ROWS, 1, LANES), f32),
            pltpu.VMEM((8, 2 * mig), f32),
            pltpu.VMEM((2, 8, 2 * mig), f32),
            pltpu.VMEM((blocks, 4, LANES, LANES), f32),
            pltpu.VMEM((blocks, 3, LANES, LANES), f32),
            pltpu.VMEM((LANES, 2 * (FORMS - 1) * LANES), jnp.bfloat16),
            pltpu.VMEM((blocks, FORMS * LANES, 2 * LANES), jnp.bfloat16),
            pltpu.VMEM((blocks, 2, 8, LANES), f32),
            pltpu.VMEM((FORMS * LANES, 2 * LANES), f32),
            pltpu.VMEM((FORMS * LANES, 2 * LANES), f32),
            pltpu.VMEM((2, 8, LANES), f32),
            pltpu.VMEM((8, LANES), f32),
            pltpu.VMEM((total, 8, LANES), f32),
            dma((2,)),
            dma((2,)),
            dma((slots,)),
            dma((slots,)),
            dma((total,)),
            dma((total,)),
        ],
        compiler_params=pltpu.CompilerParams(collective_id=0, has_side_effects=True),
    )(*arrays)
    return pl.pallas_call(
        hand_over,
        name="hand_over",
        out_shape=(
            jax.ShapeDtypeStruct(fraction.shape, f32),
            jax.ShapeDtypeStruct((1,), f32),
            jax.ShapeDtypeStruct((1,), f32),
        ),
        in_specs=[vmem, vmem],
        out_specs=(pl.BlockSpec(memory_space=pl.ANY), smem, smem),
        scratch_shapes=[pltpu.SemaphoreType.DMA],
    )(pltpu.with_memory_space_constraint(forces, pltpu.VMEM), pltpu.with_memory_space_constraint(tally, pltpu.VMEM))


def solution(mesh):
    sizes = (mesh.shape["dx"], mesh.shape["dy"], mesh.shape["dz"])
    return jax.shard_map(
        lambda *arrays: on_device(sizes, *arrays),
        mesh=mesh,
        in_specs=(
            P(None, ("win", "dx"), "dy", "dz", None),
            P(("win", "dx"), "dy", "dz", None),
            P(("win", "dx"), "dy", "dz", None),
            P(("win", "dx"), "dy", "dz", None, None),
            P(("win", "dx"), "dy", "dz", None, None),
            P(("win", "dx"), "dy", "dz", None),
            P(),
            P(),
            P(),
            P(),
            P("win"),
        ),
        out_specs=(P(None, ("win", "dx"), "dy", "dz", None), P("win"), P("win")),
        check_vma=False,
    )
```

```python
import jax
import jax.numpy as jnp
from jax import lax
from jax.experimental import pallas as pl
from jax.experimental.pallas import tpu as pltpu
from jax.sharding import PartitionSpec as P

soft_base = 0.3
soft_alpha = 0.5
charge_base = 0.3
charge_alpha = 0.5
coulomb = 0.1
LANES = 128
MESH = pl.DeviceIdType.MESH
COLS = 9


def steps_of(count):
    return {1: (0,), 2: (0, 1)}.get(count, (-1, 0, 1))


def slot_step(step, count):
    if count == 1:
        return step * 0
    if count == 2:
        return step * step
    return step + 1


def thirds(value):
    high = value.astype(jnp.bfloat16).astype(jnp.float32)
    rest = value - high
    middle = rest.astype(jnp.bfloat16).astype(jnp.float32)
    return jnp.concatenate([high, middle, rest - middle], axis=0)


def joined(value):
    return value[0:8] + value[8:16] + value[16:24]


def step_kernel(
    sizes,
    *refs,
):
    inputs, refs = refs[:11], refs[11:]
    force_ref, tally_ref, *refs = refs
    staged, (load_sem, *refs) = refs[:11], refs[11:]
    (
        edge_ref,
        coupling_ref,
        sigma_ref,
        depth_ref,
        charge_ref,
        listed_ref,
        count_ref,
        fraction_ref,
        type_ref,
        flag_ref,
        leaving_ref,
    ) = staged
    (
        ghost_ref,
        outgoing,
        incoming,
        own_cols,
        force_acc,
        params,
        self_ref,
        sums_ref,
        tile,
        gathered,
        mig_send,
        mig_recv,
        send_sem,
        recv_sem,
        sum_send,
        sum_recv,
    ) = refs
    nx, ny, nz = sizes
    atoms = fraction_ref.shape[-1]
    spacing = float(atoms) ** (1.0 / 3.0)
    me = (lax.axis_index("dx"), lax.axis_index("dy"), lax.axis_index("dz"))

    def device(step):
        return {
            name: lax.rem(place + by + count, count)
            for name, place, by, count in zip(("dx", "dy", "dz"), me, step, sizes)
        }

    offsets = [(a, b, c) for a in steps_of(nx) for b in steps_of(ny) for c in steps_of(nz)]
    others = [o for o in offsets if any(o)]

    def slot(o):
        return (
            slot_step(o[0], nx) * len(steps_of(ny)) + slot_step(o[1], ny)
        ) * len(steps_of(nz)) + slot_step(o[2], nz)

    barrier = pltpu.get_barrier_semaphore()
    total = nx * ny * nz
    my_id = (me[0] * ny + me[1]) * nz + me[2]

    def window_device(k):
        return {
            "dx": lax.div(k, ny * nz),
            "dy": lax.rem(lax.div(k, nz), ny),
            "dz": lax.rem(k, nz),
        }

    @pl.loop(1, total)
    def _(by):
        pl.semaphore_signal(
            barrier,
            inc=1,
            device_id=window_device(lax.rem(my_id + by, total)),
            device_id_type=MESH,
        )

    loads = [
        pltpu.make_async_copy(source, target, load_sem.at[k])
        for k, (source, target) in enumerate(zip(inputs, staged))
    ]
    for load in loads:
        load.start()
    for load in loads:
        load.wait()

    own = ghost_ref.at[slot((0, 0, 0))]
    edge = [edge_ref[k] * (spacing * 3.0**-0.5) for k in range(3)]
    rows = [fraction_ref[k, 0, 0] * edge[k] for k in range(3)]
    rows += [type_ref[0, 0].astype(jnp.float32), flag_ref[0, 0].astype(jnp.float32)]
    payload = jnp.concatenate(rows + [jnp.zeros((3, atoms), jnp.float32)], axis=0)
    leave = leaving_ref[0, 0, 0]
    mig = leave.shape[1]
    slots_in = jnp.concatenate([leave[0:1], leave[1:2]], axis=1)
    slots_out = jnp.concatenate([leave[1:2], leave[0:1]], axis=1)
    place = lax.broadcasted_iota(jnp.int32, (atoms, 2 * mig), 0)
    hot_in = (place == slots_in).astype(jnp.float32).astype(jnp.bfloat16)
    hot_out = (place == slots_out).astype(jnp.float32).astype(jnp.bfloat16)
    lane = lax.broadcasted_iota(jnp.int32, (8, 2 * mig), 1)
    first = lax.broadcasted_iota(jnp.int32, (8, 2 * mig), 0) == 0
    shift = jnp.where(first, jnp.where(lane < mig, edge[0], -edge[0]), 0.0)
    leavers = joined(
        jnp.dot(thirds(payload).astype(jnp.bfloat16), hot_out, preferred_element_type=jnp.float32)
    )
    outgoing[...] = leavers + shift

    def spread(value):
        return lax.dot_general(
            value.astype(jnp.bfloat16),
            hot_in,
            (((1,), (1,)), ((), ())),
            preferred_element_type=jnp.float32,
        )

    gone = spread(jnp.ones((8, 2 * mig), jnp.float32))

    pl.semaphore_wait(barrier, total - 1)
    moves = []
    for side, by in ((0, 1), (1, -1)):
        move = pltpu.make_async_remote_copy(
            src_ref=outgoing,
            dst_ref=incoming.at[side],
            send_sem=mig_send.at[side],
            recv_sem=mig_recv.at[side],
            device_id=device((by, 0, 0)),
            device_id_type=MESH,
        )
        move.start()
        moves.append(move)
    for move in moves:
        move.wait()
    merged = jnp.where(lane < mig, incoming[1], incoming[0])
    moved = jnp.where(gone > 0.5, joined(spread(thirds(merged))), payload)
    for r in range(5):
        own[r] = moved[r : r + 1]
    copies = []
    for k, o in enumerate(sorted(others, key=lambda o: -sum(map(abs, o)))):
        copy = pltpu.make_async_remote_copy(
            src_ref=own,
            dst_ref=ghost_ref.at[slot(o)],
            send_sem=send_sem.at[k],
            recv_sem=recv_sem.at[k],
            device_id=device(tuple(-x for x in o)),
            device_id_type=MESH,
        )
        copy.start()
        copies.append((copy, slot(o)))

    blocks = atoms // LANES
    lam = coupling_ref[0]
    own_slot = slot((0, 0, 0))
    ones = jnp.ones((8, LANES), jnp.bfloat16)
    for k in range(3):
        sums_ref[k] = jnp.zeros((8, LANES), jnp.float32)

    lane = lax.broadcasted_iota(jnp.int32, (1, LANES), 1)
    tables = [jnp.zeros((1, LANES), jnp.float32)] * 3
    for k in range(sigma_ref.shape[0]):
        hit = lane == k
        tables = [
            jnp.where(hit, ref[k], table)
            for ref, table in zip((sigma_ref, depth_ref, charge_ref), tables)
        ]
    table = jnp.concatenate(
        [tables[0] * (0.5 * 3.0**-0.5), jnp.sqrt(tables[1]) * 2.0, tables[2]]
        + [tables[2] * 0.0] * 5,
        axis=0,
    )
    kinds = sigma_ref.shape[0]
    table_parts = thirds(table[:, :kinds]).astype(jnp.bfloat16)
    kind_row = lax.broadcasted_iota(jnp.int32, (kinds, atoms), 0).astype(jnp.float32)

    def look_up(place):
        onehot = (kind_row == ghost_ref[place, 3]).astype(jnp.float32).astype(jnp.bfloat16)
        found = joined(jnp.dot(table_parts, onehot, preferred_element_type=jnp.float32))
        rows = [ghost_ref[place, r] for r in range(3)]
        rows += [found[0:3], ghost_ref[place, 4], found[3:4]]
        whole = jnp.concatenate(rows, axis=0)
        for q in range(blocks):
            params[place * blocks + q] = whole[:, q * LANES : (q + 1) * LANES]

    look_up(own_slot)
    picks = (
        lax.broadcasted_iota(jnp.int32, (24, COLS * LANES), 0) % 8
        == lax.broadcasted_iota(jnp.int32, (24, COLS * LANES), 1) // LANES
    ).astype(jnp.float32).astype(jnp.bfloat16)

    def graded(flag):
        return [soft_base + (soft_alpha * lam) * flag, 1.0 - lam * flag]

    deep = lax.broadcasted_iota(jnp.int32, (8, LANES), 0)
    for q in range(blocks):
        rows = params[own_slot * blocks + q]
        rows = jnp.concatenate([rows[0:5], rows[5:6] * (0.5 * coulomb), rows[6:8]], axis=0)
        cols = thirds(rows).T.astype(jnp.bfloat16)
        wide = jnp.dot(cols, picks, preferred_element_type=jnp.float32)
        for r in range(7):
            own_cols[q, r] = wide[:, r * LANES : (r + 1) * LANES]
        for r, col in enumerate(graded(own_cols[q, 6])):
            own_cols[q, 7 + r] = col
        flag = rows[6:7]
        (soft,) = graded(flag)[:1]
        ratio = 1.0 / soft
        root = lax.rsqrt(soft)
        plain = params[own_slot * blocks + q][5:6]
        electric = (coulomb * root) * plain * plain
        first = rows[4:5] * rows[4:5] * ratio
        second = first * ratio
        alone = second - first
        slope = (second + alone) * ratio + 0.5 * electric * (root * root)
        alone = alone + electric
        for k, value in enumerate((alone, flag * alone, flag * slope)):
            self_ref[q, k] = jnp.where(deep == 0, value, 0.0)
    for q in range(blocks):
        for k in range(3):
            force_acc[q, k] = jnp.zeros((LANES, LANES), jnp.float32)

    for copy, place in copies:
        copy.wait()
        look_up(place)

    width = listed_ref.shape[-1]
    together = 2 if width % 2 == 0 else 1
    groups = 8 if width % (8 * together) == 0 else 1

    def entry(q, e):
        listed = listed_ref[q, 0, e]
        left = jnp.minimum(jnp.maximum(count_ref[0, 0, 0, q] - e, 0), 1)
        used = left.astype(jnp.float32)
        apart = jnp.abs(listed - (13 * blocks + q))
        itself = ((1 - jnp.minimum(apart, 1)) * left).astype(jnp.float32)
        image = lax.div(listed, blocks)
        a = lax.div(image, 9) - 1
        b = lax.rem(lax.div(image, 3), 3) - 1
        c = lax.rem(image, 3) - 1
        where_from = (
            slot_step(a, nx) * len(steps_of(ny)) + slot_step(b, ny)
        ) * len(steps_of(nz)) + slot_step(c, nz)
        other = params[where_from * blocks + lax.rem(listed, blocks)]
        rows = []
        for r in range(7):
            row = other[r : r + 1]
            if r < 3:
                row = row + (a, b, c)[r].astype(jnp.float32) * edge[r]
            if 4 <= r < 6:
                row = row * used
            rows.append(row)
        rows += graded(rows[6])
        return [jnp.broadcast_to(row, (8, LANES)) for row in rows], itself

    @pl.loop(0, blocks)
    def _(q):
        def turn(step):
            others = [entry(q, step * together + k) for k in range(together)]
            tot, tot_p, tot_k = (
                sum(-itself * self_ref[q, k] for _, itself in others) for k in range(3)
            )
            for g in range(LANES // 8):
                at = pl.ds(g * 8, 8)
                xi, yi, zi, hi, ei, qi, pi, si, wi = (own_cols[q, r, at] for r in range(COLS))
                forces = None
                for (xj, yj, zj, hj, ej, qj, pj, sj, wj), _ in others:
                    dx, dy, dz = xi - xj, yi - yj, zi - zj
                    r2 = dx * dx + dy * dy + dz * dz
                    sig = hi + hj
                    s2 = sig * sig
                    s6 = s2 * s2 * s2
                    soft = jnp.maximum(si, sj)
                    p = jnp.maximum(pi, pj)
                    r4 = r2 * r2
                    inv = 1.0 / (s6 * soft + r4 * r2)
                    u = lax.rsqrt(3.0 * r2 + soft)
                    half = (qi * qj) * u
                    ec = half + half
                    half = half * (u * u)
                    t = s6 * inv
                    first = (ei * ej) * t
                    second = first * t
                    v = second - first
                    m = second + v
                    v = v + ec
                    kk = m * t + half
                    fs = jnp.minimum(wi, wj) * (m * (r4 * inv) + half)
                    tot = tot + v
                    tot_p = tot_p + p * v
                    tot_k = tot_k + p * kk
                    new = [fs * dx, fs * dy, fs * dz]
                    forces = new if forces is None else [x + y for x, y in zip(forces, new)]
                for k in range(3):
                    force_acc[q, k, at] += forces[k]
            for k, value in enumerate((tot, tot_p, tot_k)):
                sums_ref[k] += value

        @pl.loop(0, width // (together * groups))
        def _(step):
            for k in range(groups):
                turn(step * groups + k)

    folded = [jnp.sum(sums_ref[k], axis=0, keepdims=True) for k in range(3)]
    folded.append(jnp.zeros((5, LANES), jnp.float32))
    mine = jnp.concatenate(folded, axis=0)
    tile[...] = mine
    gathered[my_id] = mine

    def share(by):
        return pltpu.make_async_remote_copy(
            src_ref=tile,
            dst_ref=gathered.at[my_id],
            send_sem=sum_send.at[by],
            recv_sem=sum_recv.at[by],
            device_id=window_device(lax.rem(my_id + by, total)),
            device_id_type=MESH,
        )

    @pl.loop(1, total)
    def _(by):
        share(by).start()

    for q in range(blocks):
        for k in range(3):
            whole = force_acc[q, k]
            high = whole.astype(jnp.bfloat16)
            low = (whole - high.astype(jnp.float32)).astype(jnp.bfloat16)
            reduced = sum(
                lax.dot_general(
                    ones, part, (((1,), (1,)), ((), ())), preferred_element_type=jnp.float32
                )
                for part in (high, low)
            )
            force_ref[k, 0, 0, :, q * LANES : (q + 1) * LANES] = (2.0 * 3.0**0.5) * reduced[0:1]

    @pl.loop(1, total)
    def _(by):
        share(by).wait()

    summed = jnp.sum(gathered[...], axis=0)
    parts = [jnp.sum(summed[k : k + 1]) for k in range(3)]
    scale = 0.5 / float(atoms * total)
    rows = lax.broadcasted_iota(jnp.int32, (8, LANES), 0)
    energy = scale * (parts[0] - lam * parts[1])
    dhdl = -scale * (parts[1] + (0.5 * (1.0 - lam)) * parts[2])
    tally_ref[...] = jnp.where(rows == 0, energy, dhdl)


def hand_over(force_in, tally_in, force_ref, energy_ref, dhdl_ref, sem):
    copy = pltpu.make_async_copy(force_in, force_ref, sem)
    copy.start()
    energy_ref[0] = tally_in[0, 0]
    dhdl_ref[0] = tally_in[1, 0]
    copy.wait()


def on_device(sizes, fraction, atom_type, perturbed, leaving, neighbours, counts,
              sigma_table, depth_table, charge_table, domain_edge, coupling):
    nx, ny, nz = sizes
    atoms = fraction.shape[-1]
    mig = leaving.shape[-1]
    slots = len(steps_of(nx)) * len(steps_of(ny)) * len(steps_of(nz))
    smem = pl.BlockSpec(memory_space=pltpu.SMEM)
    vmem = pl.BlockSpec(memory_space=pltpu.VMEM)
    f32 = jnp.float32

    def bound(kernel, *values):
        return lambda *refs: kernel(*values, *refs)

    blocks = atoms // LANES
    total = nx * ny * nz
    dma = pltpu.SemaphoreType.DMA
    arrays = (
        domain_edge,
        coupling,
        sigma_table,
        depth_table,
        charge_table,
        neighbours.reshape(blocks, 1, -1),
        counts,
        fraction,
        atom_type,
        perturbed,
        leaving,
    )
    forces, tally = pl.pallas_call(
        bound(step_kernel, sizes),
        name="step",
        out_shape=(pltpu.VMEM(fraction.shape, f32), pltpu.VMEM((8, LANES), f32)),
        in_specs=[pl.BlockSpec(memory_space=pl.ANY)] * 11,
        out_specs=(vmem, vmem),
        scratch_shapes=[
            *(pltpu.SMEM(x.shape, x.dtype) for x in arrays[:7]),
            *(pltpu.VMEM(x.shape, x.dtype) for x in arrays[7:]),
            dma((11,)),
            pltpu.VMEM((slots, 5, 1, atoms), f32),
            pltpu.VMEM((8, 2 * mig), f32),
            pltpu.VMEM((2, 8, 2 * mig), f32),
            pltpu.VMEM((blocks, COLS, LANES, LANES), f32),
            pltpu.VMEM((blocks, 3, LANES, LANES), f32),
            pltpu.VMEM((slots * blocks, 8, LANES), f32),
            pltpu.VMEM((blocks, 3, 8, LANES), f32),
            pltpu.VMEM((3, 8, LANES), f32),
            pltpu.VMEM((8, LANES), f32),
            pltpu.VMEM((total, 8, LANES), f32),
            dma((2,)),
            dma((2,)),
            dma((slots,)),
            dma((slots,)),
            dma((total,)),
            dma((total,)),
        ],
        compiler_params=pltpu.CompilerParams(collective_id=0, has_side_effects=True),
    )(*arrays)
    return pl.pallas_call(
        hand_over,
        name="hand_over",
        out_shape=(
            jax.ShapeDtypeStruct(fraction.shape, f32),
            jax.ShapeDtypeStruct((1,), f32),
            jax.ShapeDtypeStruct((1,), f32),
        ),
        in_specs=[vmem, vmem],
        out_specs=(pl.BlockSpec(memory_space=pl.ANY), smem, smem),
        scratch_shapes=[pltpu.SemaphoreType.DMA],
    )(pltpu.with_memory_space_constraint(forces, pltpu.VMEM), pltpu.with_memory_space_constraint(tally, pltpu.VMEM))


def solution(mesh):
    sizes = (mesh.shape["dx"], mesh.shape["dy"], mesh.shape["dz"])
    return jax.shard_map(
        lambda *arrays: on_device(sizes, *arrays),
        mesh=mesh,
        in_specs=(
            P(None, ("win", "dx"), "dy", "dz", None),
            P(("win", "dx"), "dy", "dz", None),
            P(("win", "dx"), "dy", "dz", None),
            P(("win", "dx"), "dy", "dz", None, None),
            P(("win", "dx"), "dy", "dz", None, None),
            P(("win", "dx"), "dy", "dz", None),
            P(),
            P(),
            P(),
            P(),
            P("win"),
        ),
        out_specs=(P(None, ("win", "dx"), "dy", "dz", None), P("win"), P("win")),
        check_vma=False,
    )
```

```python
import jax
import jax.numpy as jnp
from jax import lax
from jax.experimental import pallas as pl
from jax.experimental.pallas import tpu as pltpu
from jax.sharding import PartitionSpec as P

soft_base = 0.3
soft_alpha = 0.5
charge_base = 0.3
charge_alpha = 0.5
coulomb = 0.1
LANES = 128
MESH = pl.DeviceIdType.MESH
COLS = 9
ROWS = 5


def steps_of(count):
    return {1: (0,), 2: (0, 1)}.get(count, (-1, 0, 1))


def far_steps(count):
    return {1: (), 2: (), 3: (), 4: (2,)}.get(count, (2, -2))


def slot_step(step, count):
    if count == 1:
        return step * 0
    if count == 2:
        return step * step
    return step + 1


def thirds(value):
    high = value.astype(jnp.bfloat16).astype(jnp.float32)
    rest = value - high
    middle = rest.astype(jnp.bfloat16).astype(jnp.float32)
    return jnp.concatenate([high, middle, rest - middle], axis=0)


def joined(value):
    return value[0:8] + value[8:16] + value[16:24]


def step_kernel(
    sizes,
    *refs,
):
    inputs, refs = refs[:11], refs[11:]
    force_ref, tally_ref, *refs = refs
    staged, (load_sem, *refs) = refs[:11], refs[11:]
    (
        edge_ref,
        coupling_ref,
        sigma_ref,
        depth_ref,
        charge_ref,
        listed_ref,
        count_ref,
        fraction_ref,
        type_ref,
        flag_ref,
        leaving_ref,
    ) = staged
    (
        ghost_ref,
        far_ref,
        hot_ref,
        own_cols,
        force_acc,
        params,
        self_ref,
        sums_ref,
        tile,
        gathered,
        far_send,
        far_recv,
        send_sem,
        recv_sem,
        sum_send,
        sum_recv,
    ) = refs
    nx, ny, nz = sizes
    atoms = fraction_ref.shape[-1]
    spacing = float(atoms) ** (1.0 / 3.0)
    me = (lax.axis_index("dx"), lax.axis_index("dy"), lax.axis_index("dz"))

    def device(step):
        return {
            name: lax.rem(place + by + count, count)
            for name, place, by, count in zip(("dx", "dy", "dz"), me, step, sizes)
        }

    offsets = [(a, b, c) for a in steps_of(nx) for b in steps_of(ny) for c in steps_of(nz)]
    others = [o for o in offsets if any(o)]

    def slot(o):
        return (
            slot_step(o[0], nx) * len(steps_of(ny)) + slot_step(o[1], ny)
        ) * len(steps_of(nz)) + slot_step(o[2], nz)

    barrier = pltpu.get_barrier_semaphore()
    total = nx * ny * nz
    my_id = (me[0] * ny + me[1]) * nz + me[2]

    def window_device(k):
        return {
            "dx": lax.div(k, ny * nz),
            "dy": lax.rem(lax.div(k, nz), ny),
            "dz": lax.rem(k, nz),
        }

    @pl.loop(1, total)
    def _(by):
        pl.semaphore_signal(
            barrier,
            inc=1,
            device_id=window_device(lax.rem(my_id + by, total)),
            device_id_type=MESH,
        )

    loads = [
        pltpu.make_async_copy(source, target, load_sem.at[k])
        for k, (source, target) in enumerate(zip(inputs, staged))
    ]
    for load in loads:
        load.start()
    for load in loads:
        load.wait()

    own = ghost_ref.at[slot((0, 0, 0))]
    edge = [edge_ref[k] * (spacing * 3.0**-0.5) for k in range(3)]
    rows = [fraction_ref[k, 0, 0] * edge[k] for k in range(3)]
    rows += [type_ref[0, 0].astype(jnp.float32), flag_ref[0, 0].astype(jnp.float32)]
    payload = jnp.concatenate(rows + [jnp.zeros((3, atoms), jnp.float32)], axis=0)
    leave = leaving_ref[0, 0, 0]
    mig = leave.shape[1]
    slots_in = jnp.concatenate([leave[0:1], leave[1:2]], axis=1)
    slots_out = jnp.concatenate([leave[1:2], leave[0:1]], axis=1)
    place = lax.broadcasted_iota(jnp.int32, (atoms, 2 * mig), 0)
    hot_out = (place == slots_out).astype(jnp.float32).astype(jnp.bfloat16)
    lane = lax.broadcasted_iota(jnp.int32, (8, 2 * mig), 1)
    deep = lax.broadcasted_iota(jnp.int32, (8, 2 * mig), 0)
    shift = jnp.where(deep == 0, jnp.where(lane < mig, edge[0], -edge[0]), 0.0)
    leavers = joined(
        jnp.dot(thirds(payload).astype(jnp.bfloat16), hot_out, preferred_element_type=jnp.float32)
    )
    leavers = leavers + shift
    blocks = atoms // LANES
    body = blocks * ROWS
    per_row = LANES // (2 * mig)
    extras = -(-(ROWS + 1) // per_row)
    for q in range(blocks):
        for r in range(ROWS):
            own[q * ROWS + r] = payload[r : r + 1, q * LANES : (q + 1) * LANES]
    parts = [leavers[r : r + 1] for r in range(ROWS)] + [slots_in.astype(jnp.float32)]
    parts += [parts[0] * 0.0] * (extras * per_row - ROWS - 1)
    for r in range(extras):
        own[body + r] = jnp.concatenate(parts[r * per_row : (r + 1) * per_row], axis=1)

    pl.semaphore_wait(barrier, total - 1)

    def passing(source, target, place, k):
        return pltpu.make_async_remote_copy(
            src_ref=source,
            dst_ref=ghost_ref.at[place],
            send_sem=send_sem.at[k],
            recv_sem=recv_sem.at[place],
            device_id=device(target),
            device_id_type=MESH,
        )

    fars = far_steps(nx)
    ends = [(a, b, c) for a in fars for b in steps_of(ny) for c in steps_of(nz)]

    def far_slot(a, b, c):
        which = (2 - a) // 4 if len(fars) > 1 else 0
        return (which * len(steps_of(ny)) + slot_step(b, ny)) * len(steps_of(nz)) + slot_step(c, nz)

    def far_copy(k, target, here):
        return pltpu.make_async_remote_copy(
            src_ref=own.at[pl.ds(body, extras)],
            dst_ref=far_ref.at[here],
            send_sem=far_send.at[k],
            recv_sem=far_recv.at[here],
            device_id=device(target),
            device_id_type=MESH,
        )

    far_copies = [
        far_copy(k, (a, b, c), far_slot(-a if len(fars) > 1 else a, -b, -c))
        for k, (a, b, c) in enumerate(ends)
    ]
    for copy in far_copies:
        copy.start()

    if nx > 2:
        toward = 2 * lax.div(2 * me[0], nx) - 1
        reach = [toward, -toward]
    else:
        reach = [x for x in steps_of(nx) if x]
    sides = sorted((b for b in steps_of(ny)), key=lambda b: -abs(b))
    plan = [(a, b) for a in reach for b in sides] + [(0, b) for b in sides if b]
    up = [c for c in steps_of(nz) if c]
    sends = []
    for a, b in plan:
        sends.append(passing(own, (a, b, 0), slot((-a, -b, 0)), len(sends)))
        sends[-1].start()
    for c in up:
        sends.append(passing(own, (0, 0, -c), slot((0, 0, c)), len(sends)))
        sends[-1].start()

    lam = coupling_ref[0]
    own_slot = slot((0, 0, 0))
    ones = jnp.ones((8, LANES), jnp.bfloat16)
    for k in range(3):
        sums_ref[k] = jnp.zeros((8, LANES), jnp.float32)

    lane = lax.broadcasted_iota(jnp.int32, (1, LANES), 1)
    tables = [jnp.zeros((1, LANES), jnp.float32)] * 3
    for k in range(sigma_ref.shape[0]):
        hit = lane == k
        tables = [
            jnp.where(hit, ref[k], table)
            for ref, table in zip((sigma_ref, depth_ref, charge_ref), tables)
        ]
    table = jnp.concatenate(
        [tables[0] * (0.5 * 3.0**-0.5), jnp.sqrt(tables[1]) * 2.0, tables[2]]
        + [tables[2] * 0.0] * 5,
        axis=0,
    )
    kinds = sigma_ref.shape[0]
    table_parts = thirds(table[:, :kinds]).astype(jnp.bfloat16)
    kind_row = lax.broadcasted_iota(jnp.int32, (kinds, atoms), 0).astype(jnp.float32)

    low_side = jnp.where(lax.broadcasted_iota(jnp.int32, (1, 2 * mig), 1) < mig, 1, -1)
    atom_lane = lax.broadcasted_iota(jnp.int32, (2 * mig, atoms), 1).astype(jnp.float32)
    one_row = jnp.ones((1, 2 * mig), jnp.float32)

    def extra_rows(a, b, c):
        far = not isinstance(a, int) or abs(a) == 2
        if far and fars:
            found = [far_ref[far_slot(a, b, c), r] for r in range(extras)]
        else:
            if far:
                a = -a // 2 if nx == 3 else 0
            found = [ghost_ref[slot((a, b, c)), body + r] for r in range(extras)]
        return [
            found[r // per_row][:, (r % per_row) * 2 * mig : (r % per_row + 1) * 2 * mig]
            for r in range(ROWS + 1)
        ]

    def prepare(a, b, c):
        place = slot((a, b, c))
        rows = [
            jnp.concatenate([ghost_ref[place, q * ROWS + r] for q in range(blocks)], axis=1)
            for r in range(ROWS)
        ]
        found = joined(
            jnp.dot(
                table_parts,
                (kind_row == rows[3]).astype(jnp.float32).astype(jnp.bfloat16),
                preferred_element_type=jnp.float32,
            )
        )
        whole = jnp.concatenate(rows[0:3] + [found[0:3], rows[4], found[3:4]], axis=0)
        for q in range(blocks):
            params[place * blocks + q] = whole[:, q * LANES : (q + 1) * LANES]
        at = ROWS % per_row
        slots_here = ghost_ref[place, body + ROWS // per_row][:, at * 2 * mig : (at + 1) * 2 * mig]
        column = jnp.broadcast_to(slots_here, (8, 2 * mig)).T[:, 0:1]
        hot = jnp.broadcast_to(column, (2 * mig, atoms)) == atom_lane
        hot_ref[place] = hot.astype(jnp.float32).astype(jnp.bfloat16)

    def patch(a, b, c):
        place = slot((a, b, c))
        if isinstance(a, int) and a == 0:
            near, away = extra_rows(1, b, c), extra_rows(-1, b, c)
            pick = low_side > 0
        else:
            near, away = extra_rows(2 * a, b, c), extra_rows(0, b, c)
            pick = low_side * a > 0
        rows = [jnp.where(pick, x, y) for x, y in zip(near[:ROWS], away[:ROWS])]
        found = joined(
            jnp.dot(
                table_parts,
                (kind_row[:, : 2 * mig] == rows[3]).astype(jnp.float32).astype(jnp.bfloat16),
                preferred_element_type=jnp.float32,
            )
        )
        whole = jnp.concatenate(rows[0:3] + [found[0:3], rows[4], one_row], axis=0)
        spread = joined(
            jnp.dot(
                thirds(whole).astype(jnp.bfloat16),
                hot_ref[place],
                preferred_element_type=jnp.float32,
            )
        )
        for q in range(blocks):
            new = spread[:, q * LANES : (q + 1) * LANES]
            at = place * blocks + q
            params[at] = jnp.where(new[7:8] > 0.5, new, params[at])

    picks = (
        lax.broadcasted_iota(jnp.int32, (24, COLS * LANES), 0) % 8
        == lax.broadcasted_iota(jnp.int32, (24, COLS * LANES), 1) // LANES
    ).astype(jnp.float32).astype(jnp.bfloat16)

    def graded(flag):
        return [soft_base + (soft_alpha * lam) * flag, 1.0 - lam * flag]

    deep = lax.broadcasted_iota(jnp.int32, (8, LANES), 0)
    def own_side():
        for q in range(blocks):
            rows = params[own_slot * blocks + q]
            rows = jnp.concatenate([rows[0:5], rows[5:6] * (0.5 * coulomb), rows[6:8]], axis=0)
            cols = thirds(rows).T.astype(jnp.bfloat16)
            wide = jnp.dot(cols, picks, preferred_element_type=jnp.float32)
            for r in range(7):
                own_cols[q, r] = wide[:, r * LANES : (r + 1) * LANES]
            for r, col in enumerate(graded(own_cols[q, 6])):
                own_cols[q, 7 + r] = col
            flag = rows[6:7]
            (soft,) = graded(flag)[:1]
            ratio = 1.0 / soft
            root = lax.rsqrt(soft)
            plain = params[own_slot * blocks + q][5:6]
            electric = (coulomb * root) * plain * plain
            first = rows[4:5] * rows[4:5] * ratio
            second = first * ratio
            alone = second - first
            slope = (second + alone) * ratio + 0.5 * electric * (root * root)
            alone = alone + electric
            for k, value in enumerate((alone, flag * alone, flag * slope)):
                self_ref[q, k] = jnp.where(deep == 0, value, 0.0)

    for q in range(blocks):
        for k in range(3):
            force_acc[q, k] = jnp.zeros((LANES, LANES), jnp.float32)

    def arrive(a, b):
        here = slot((a, b, 0))
        passing(own, (a, b, 0), here, 0).wait_recv()
        for c in up:
            sends.append(passing(ghost_ref.at[here], (0, 0, -c), slot((a, b, c)), len(sends)))
            sends[-1].start()

    def across(a, b):
        for c in up:
            passing(own, (0, 0, -c), slot((a, b, c)), 0).wait_recv()
            prepare(a, b, c)

    nearest = sides[::-1]
    prepare(0, 0, 0)
    for b in nearest:
        if b:
            arrive(0, b)
            prepare(0, b, 0)
    across(0, 0)
    for a in reach[1:]:
        for b in nearest:
            arrive(a, b)
            prepare(a, b, 0)
    for b in nearest:
        if b:
            across(0, b)
    for a in reach[1:]:
        for b in nearest:
            across(a, b)
    for o in ends:
        far_copy(0, o, far_slot(*o)).wait_recv()
    for a in reach[1:]:
        for b in nearest:
            for c in steps_of(nz):
                patch(a, b, c)
    for a in reach[:1]:
        for b in nearest:
            arrive(a, b)
    for b in nearest:
        for a in reach[:1]:
            prepare(a, b, 0)
            patch(a, b, 0)
        patch(0, b, 0)
    own_side()
    for b in nearest:
        for a in reach[:1]:
            across(a, b)
        for c in up:
            for a in [0] + reach[:1]:
                patch(a, b, c)

    width = listed_ref.shape[-1]
    together = 2 if width % 2 == 0 else 1
    groups = 8 if width % (8 * together) == 0 else 1

    def entry(q, e):
        listed = listed_ref[q, 0, e]
        left = jnp.minimum(jnp.maximum(count_ref[0, 0, 0, q] - e, 0), 1)
        used = left.astype(jnp.float32)
        apart = jnp.abs(listed - (13 * blocks + q))
        itself = ((1 - jnp.minimum(apart, 1)) * left).astype(jnp.float32)
        image = lax.div(listed, blocks)
        a = lax.div(image, 9) - 1
        b = lax.rem(lax.div(image, 3), 3) - 1
        c = lax.rem(image, 3) - 1
        where_from = (
            slot_step(a, nx) * len(steps_of(ny)) + slot_step(b, ny)
        ) * len(steps_of(nz)) + slot_step(c, nz)
        other = params[where_from * blocks + lax.rem(listed, blocks)]
        rows = []
        for r in range(7):
            row = other[r : r + 1]
            if r < 3:
                row = row + (a, b, c)[r].astype(jnp.float32) * edge[r]
            if 4 <= r < 6:
                row = row * used
            rows.append(row)
        rows += graded(rows[6])
        return [jnp.broadcast_to(row, (8, LANES)) for row in rows], itself

    @pl.loop(0, blocks)
    def _(q):
        def turn(step):
            others = [entry(q, step * together + k) for k in range(together)]
            tot, tot_p, tot_k = (
                sum(-itself * self_ref[q, k] for _, itself in others) for k in range(3)
            )
            for g in range(LANES // 8):
                at = pl.ds(g * 8, 8)
                xi, yi, zi, hi, ei, qi, pi, si, wi = (own_cols[q, r, at] for r in range(COLS))
                forces = None
                for (xj, yj, zj, hj, ej, qj, pj, sj, wj), _ in others:
                    dx, dy, dz = xi - xj, yi - yj, zi - zj
                    r2 = dx * dx + dy * dy + dz * dz
                    sig = hi + hj
                    s2 = sig * sig
                    s6 = s2 * s2 * s2
                    soft = jnp.maximum(si, sj)
                    p = jnp.maximum(pi, pj)
                    r4 = r2 * r2
                    inv = 1.0 / (s6 * soft + r4 * r2)
                    u = lax.rsqrt(3.0 * r2 + soft)
                    half = (qi * qj) * u
                    ec = half + half
                    half = half * (u * u)
                    t = s6 * inv
                    first = (ei * ej) * t
                    second = first * t
                    v = second - first
                    m = second + v
                    v = v + ec
                    kk = m * t + half
                    fs = jnp.minimum(wi, wj) * (m * (r4 * inv) + half)
                    tot = tot + v
                    tot_p = tot_p + p * v
                    tot_k = tot_k + p * kk
                    new = [fs * dx, fs * dy, fs * dz]
                    forces = new if forces is None else [x + y for x, y in zip(forces, new)]
                for k in range(3):
                    force_acc[q, k, at] += forces[k]
            for k, value in enumerate((tot, tot_p, tot_k)):
                sums_ref[k] += value

        @pl.loop(0, width // (together * groups))
        def _(step):
            for k in range(groups):
                turn(step * groups + k)

    part = LANES // 4

    def narrowed(row):
        row = row + pltpu.roll(row, LANES // 2, 1)
        return row + pltpu.roll(row, part, 1)

    folded = [narrowed(jnp.sum(sums_ref[k], axis=0, keepdims=True)) for k in range(3)]
    lane = lax.broadcasted_iota(jnp.int32, (1, LANES), 1)
    mine = jnp.where(lane < part, folded[0], jnp.where(lane < 2 * part, folded[1], folded[2]))
    tile[...] = mine
    gathered[my_id] = mine

    def share(by):
        return pltpu.make_async_remote_copy(
            src_ref=tile,
            dst_ref=gathered.at[my_id],
            send_sem=sum_send.at[by],
            recv_sem=sum_recv.at[by],
            device_id=window_device(lax.rem(my_id + by, total)),
            device_id_type=MESH,
        )

    @pl.loop(1, total)
    def _(by):
        share(by).start()

    for q in range(blocks):
        for k in range(3):
            whole = force_acc[q, k]
            high = whole.astype(jnp.bfloat16)
            low = (whole - high.astype(jnp.float32)).astype(jnp.bfloat16)
            reduced = sum(
                lax.dot_general(
                    ones, part, (((1,), (1,)), ((), ())), preferred_element_type=jnp.float32
                )
                for part in (high, low)
            )
            force_ref[k, 0, 0, :, q * LANES : (q + 1) * LANES] = (2.0 * 3.0**0.5) * reduced[0:1]

    for copy in sends + far_copies:
        copy.wait_send()

    @pl.loop(1, total)
    def _(by):
        share(by).wait()

    summed = jnp.sum(gathered[...], axis=0)
    parts = [
        jnp.sum(jnp.where(lax.div(lane, part) == k, summed, 0.0)) for k in range(3)
    ]
    scale = 0.5 / float(atoms * total)
    rows = lax.broadcasted_iota(jnp.int32, (8, LANES), 0)
    energy = scale * (parts[0] - lam * parts[1])
    dhdl = -scale * (parts[1] + (0.5 * (1.0 - lam)) * parts[2])
    tally_ref[...] = jnp.where(rows == 0, energy, dhdl)


def hand_over(force_in, tally_in, force_ref, energy_ref, dhdl_ref, sem):
    copy = pltpu.make_async_copy(force_in, force_ref, sem)
    copy.start()
    energy_ref[0] = tally_in[0, 0]
    dhdl_ref[0] = tally_in[1, 0]
    copy.wait()


def on_device(sizes, fraction, atom_type, perturbed, leaving, neighbours, counts,
              sigma_table, depth_table, charge_table, domain_edge, coupling):
    nx, ny, nz = sizes
    atoms = fraction.shape[-1]
    mig = leaving.shape[-1]
    slots = len(steps_of(nx)) * len(steps_of(ny)) * len(steps_of(nz))
    planar = len(steps_of(ny)) * len(steps_of(nz))
    far_slots = max(len(far_steps(nx)), 1) * planar
    extras = -(-(ROWS + 1) // (LANES // (2 * mig)))
    smem = pl.BlockSpec(memory_space=pltpu.SMEM)
    vmem = pl.BlockSpec(memory_space=pltpu.VMEM)
    f32 = jnp.float32

    def bound(kernel, *values):
        return lambda *refs: kernel(*values, *refs)

    blocks = atoms // LANES
    total = nx * ny * nz
    dma = pltpu.SemaphoreType.DMA
    arrays = (
        domain_edge,
        coupling,
        sigma_table,
        depth_table,
        charge_table,
        neighbours.reshape(blocks, 1, -1),
        counts,
        fraction,
        atom_type,
        perturbed,
        leaving,
    )
    forces, tally = pl.pallas_call(
        bound(step_kernel, sizes),
        name="step",
        out_shape=(pltpu.VMEM(fraction.shape, f32), pltpu.VMEM((8, LANES), f32)),
        in_specs=[pl.BlockSpec(memory_space=pl.ANY)] * 11,
        out_specs=(vmem, vmem),
        scratch_shapes=[
            *(pltpu.SMEM(x.shape, x.dtype) for x in arrays[:7]),
            *(pltpu.VMEM(x.shape, x.dtype) for x in arrays[7:]),
            dma((11,)),
            pltpu.VMEM((slots, blocks * ROWS + extras, 1, LANES), f32),
            pltpu.VMEM((far_slots, extras, 1, LANES), f32),
            pltpu.VMEM((slots, 2 * mig, atoms), jnp.bfloat16),
            pltpu.VMEM((blocks, COLS, LANES, LANES), f32),
            pltpu.VMEM((blocks, 3, LANES, LANES), f32),
            pltpu.VMEM((slots * blocks, 8, LANES), f32),
            pltpu.VMEM((blocks, 3, 8, LANES), f32),
            pltpu.VMEM((3, 8, LANES), f32),
            pltpu.VMEM((1, LANES), f32),
            pltpu.VMEM((total, 1, LANES), f32),
            dma((far_slots,)),
            dma((far_slots,)),
            dma((slots,)),
            dma((slots,)),
            dma((total,)),
            dma((total,)),
        ],
        compiler_params=pltpu.CompilerParams(collective_id=0, has_side_effects=True),
    )(*arrays)
    return pl.pallas_call(
        hand_over,
        name="hand_over",
        out_shape=(
            jax.ShapeDtypeStruct(fraction.shape, f32),
            jax.ShapeDtypeStruct((1,), f32),
            jax.ShapeDtypeStruct((1,), f32),
        ),
        in_specs=[vmem, vmem],
        out_specs=(pl.BlockSpec(memory_space=pl.ANY), smem, smem),
        scratch_shapes=[pltpu.SemaphoreType.DMA],
    )(pltpu.with_memory_space_constraint(forces, pltpu.VMEM), pltpu.with_memory_space_constraint(tally, pltpu.VMEM))


def solution(mesh):
    sizes = (mesh.shape["dx"], mesh.shape["dy"], mesh.shape["dz"])
    return jax.shard_map(
        lambda *arrays: on_device(sizes, *arrays),
        mesh=mesh,
        in_specs=(
            P(None, ("win", "dx"), "dy", "dz", None),
            P(("win", "dx"), "dy", "dz", None),
            P(("win", "dx"), "dy", "dz", None),
            P(("win", "dx"), "dy", "dz", None, None),
            P(("win", "dx"), "dy", "dz", None, None),
            P(("win", "dx"), "dy", "dz", None),
            P(),
            P(),
            P(),
            P(),
            P("win"),
        ),
        out_specs=(P(None, ("win", "dx"), "dy", "dz", None), P("win"), P("win")),
        check_vma=False,
    )
```

```python
import jax
import jax.numpy as jnp
from jax import lax
from jax.experimental import pallas as pl
from jax.experimental.pallas import tpu as pltpu
from jax.sharding import PartitionSpec as P

soft_base = 0.3
soft_alpha = 0.5
charge_base = 0.3
charge_alpha = 0.5
coulomb = 0.1
LANES = 128
MESH = pl.DeviceIdType.MESH
COLS = 9
ROWS = 5


def steps_of(count):
    return {1: (0,), 2: (0, 1)}.get(count, (-1, 0, 1))


def far_steps(count):
    return {1: (), 2: (), 3: (), 4: (2,)}.get(count, (2, -2))


def slot_step(step, count):
    if count == 1:
        return step * 0
    if count == 2:
        return step * step
    return step + 1


def thirds(value):
    high = value.astype(jnp.bfloat16).astype(jnp.float32)
    rest = value - high
    middle = rest.astype(jnp.bfloat16).astype(jnp.float32)
    return jnp.concatenate([high, middle, rest - middle], axis=0)


def joined(value):
    return value[0:8] + value[8:16] + value[16:24]


def step_kernel(
    sizes,
    *refs,
):
    inputs, refs = refs[:11], refs[11:]
    force_ref, tally_ref, *refs = refs
    staged, (load_sem, *refs) = refs[:11], refs[11:]
    (
        edge_ref,
        coupling_ref,
        sigma_ref,
        depth_ref,
        charge_ref,
        listed_ref,
        count_ref,
        fraction_ref,
        type_ref,
        flag_ref,
        leaving_ref,
    ) = staged
    (
        ghost_ref,
        far_ref,
        hot_ref,
        own_cols,
        force_acc,
        params,
        self_ref,
        slopes,
        sums_ref,
        tile,
        gathered,
        far_send,
        far_recv,
        send_sem,
        recv_sem,
        sum_send,
        sum_recv,
    ) = refs
    nx, ny, nz = sizes
    atoms = fraction_ref.shape[-1]
    spacing = float(atoms) ** (1.0 / 3.0)
    me = (lax.axis_index("dx"), lax.axis_index("dy"), lax.axis_index("dz"))

    def device(step):
        return {
            name: lax.rem(place + by + count, count)
            for name, place, by, count in zip(("dx", "dy", "dz"), me, step, sizes)
        }

    offsets = [(a, b, c) for a in steps_of(nx) for b in steps_of(ny) for c in steps_of(nz)]
    others = [o for o in offsets if any(o)]

    def slot(o):
        return (
            slot_step(o[0], nx) * len(steps_of(ny)) + slot_step(o[1], ny)
        ) * len(steps_of(nz)) + slot_step(o[2], nz)

    barrier = pltpu.get_barrier_semaphore()
    total = nx * ny * nz
    my_id = (me[0] * ny + me[1]) * nz + me[2]

    def window_device(k):
        return {
            "dx": lax.div(k, ny * nz),
            "dy": lax.rem(lax.div(k, nz), ny),
            "dz": lax.rem(k, nz),
        }

    @pl.loop(1, total)
    def _(by):
        pl.semaphore_signal(
            barrier,
            inc=1,
            device_id=window_device(lax.rem(my_id + by, total)),
            device_id_type=MESH,
        )

    loads = [
        pltpu.make_async_copy(source, target, load_sem.at[k])
        for k, (source, target) in enumerate(zip(inputs, staged))
    ]
    for load in loads:
        load.start()
    for load in loads:
        load.wait()

    own = ghost_ref.at[slot((0, 0, 0))]
    edge = [edge_ref[k] * (spacing * 3.0**-0.5) for k in range(3)]
    rows = [fraction_ref[k, 0, 0] * edge[k] for k in range(3)]
    rows += [type_ref[0, 0].astype(jnp.float32), flag_ref[0, 0].astype(jnp.float32)]
    payload = jnp.concatenate(rows + [jnp.zeros((3, atoms), jnp.float32)], axis=0)
    leave = leaving_ref[0, 0, 0]
    mig = leave.shape[1]
    slots_in = jnp.concatenate([leave[0:1], leave[1:2]], axis=1)
    slots_out = jnp.concatenate([leave[1:2], leave[0:1]], axis=1)
    place = lax.broadcasted_iota(jnp.int32, (atoms, 2 * mig), 0)
    hot_out = (place == slots_out).astype(jnp.float32).astype(jnp.bfloat16)
    lane = lax.broadcasted_iota(jnp.int32, (8, 2 * mig), 1)
    deep = lax.broadcasted_iota(jnp.int32, (8, 2 * mig), 0)
    shift = jnp.where(deep == 0, jnp.where(lane < mig, edge[0], -edge[0]), 0.0)
    leavers = joined(
        jnp.dot(thirds(payload).astype(jnp.bfloat16), hot_out, preferred_element_type=jnp.float32)
    )
    leavers = leavers + shift
    blocks = atoms // LANES
    body = blocks * ROWS
    per_row = LANES // (2 * mig)
    extras = -(-(ROWS + 1) // per_row)
    for q in range(blocks):
        for r in range(ROWS):
            own[q * ROWS + r] = payload[r : r + 1, q * LANES : (q + 1) * LANES]
    parts = [leavers[r : r + 1] for r in range(ROWS)] + [slots_in.astype(jnp.float32)]
    parts += [parts[0] * 0.0] * (extras * per_row - ROWS - 1)
    for r in range(extras):
        own[body + r] = jnp.concatenate(parts[r * per_row : (r + 1) * per_row], axis=1)

    pl.semaphore_wait(barrier, total - 1)

    def passing(source, target, place, k):
        return pltpu.make_async_remote_copy(
            src_ref=source,
            dst_ref=ghost_ref.at[place],
            send_sem=send_sem.at[k],
            recv_sem=recv_sem.at[place],
            device_id=device(target),
            device_id_type=MESH,
        )

    fars = far_steps(nx)
    ends = [(a, b, c) for a in fars for b in steps_of(ny) for c in steps_of(nz)]

    def far_slot(a, b, c):
        which = (2 - a) // 4 if len(fars) > 1 else 0
        return (which * len(steps_of(ny)) + slot_step(b, ny)) * len(steps_of(nz)) + slot_step(c, nz)

    def far_copy(k, target, here):
        return pltpu.make_async_remote_copy(
            src_ref=own.at[pl.ds(body, extras)],
            dst_ref=far_ref.at[here],
            send_sem=far_send.at[k],
            recv_sem=far_recv.at[here],
            device_id=device(target),
            device_id_type=MESH,
        )

    far_copies = [
        far_copy(k, (a, b, c), far_slot(-a if len(fars) > 1 else a, -b, -c))
        for k, (a, b, c) in enumerate(ends)
    ]
    for copy in far_copies:
        copy.start()

    if nx > 2:
        toward = 2 * lax.div(2 * me[0], nx) - 1
        reach = [toward, -toward]
    else:
        reach = [x for x in steps_of(nx) if x]
    sides = sorted((b for b in steps_of(ny)), key=lambda b: -abs(b))
    plan = [(a, b) for a in reach for b in sides] + [(0, b) for b in sides if b]
    up = [c for c in steps_of(nz) if c]
    sends = []
    for a, b in plan:
        sends.append(passing(own, (a, b, 0), slot((-a, -b, 0)), len(sends)))
        sends[-1].start()
    for c in up:
        sends.append(passing(own, (0, 0, -c), slot((0, 0, c)), len(sends)))
        sends[-1].start()

    lam = coupling_ref[0]
    own_slot = slot((0, 0, 0))
    ones = jnp.ones((8, LANES), jnp.bfloat16)
    for k in range(3):
        sums_ref[k] = jnp.zeros((8, LANES), jnp.float32)

    lane = lax.broadcasted_iota(jnp.int32, (1, LANES), 1)
    tables = [jnp.zeros((1, LANES), jnp.float32)] * 3
    for k in range(sigma_ref.shape[0]):
        hit = lane == k
        tables = [
            jnp.where(hit, ref[k], table)
            for ref, table in zip((sigma_ref, depth_ref, charge_ref), tables)
        ]
    table = jnp.concatenate(
        [tables[0] * (0.5 * 3.0**-0.5), jnp.sqrt(tables[1]) * 2.0, tables[2]]
        + [tables[2] * 0.0] * 5,
        axis=0,
    )
    kinds = sigma_ref.shape[0]
    table_parts = thirds(table[:, :kinds]).astype(jnp.bfloat16)
    kind_row = lax.broadcasted_iota(jnp.int32, (kinds, atoms), 0).astype(jnp.float32)

    low_side = jnp.where(lax.broadcasted_iota(jnp.int32, (1, 2 * mig), 1) < mig, 1, -1)
    atom_lane = lax.broadcasted_iota(jnp.int32, (2 * mig, atoms), 1).astype(jnp.float32)
    one_row = jnp.ones((1, 2 * mig), jnp.float32)

    def extra_rows(a, b, c):
        far = not isinstance(a, int) or abs(a) == 2
        if far and fars:
            found = [far_ref[far_slot(a, b, c), r] for r in range(extras)]
        else:
            if far:
                a = -a // 2 if nx == 3 else 0
            found = [ghost_ref[slot((a, b, c)), body + r] for r in range(extras)]
        return [
            found[r // per_row][:, (r % per_row) * 2 * mig : (r % per_row + 1) * 2 * mig]
            for r in range(ROWS + 1)
        ]

    def prepare(a, b, c):
        place = slot((a, b, c))
        rows = [
            jnp.concatenate([ghost_ref[place, q * ROWS + r] for q in range(blocks)], axis=1)
            for r in range(ROWS)
        ]
        found = joined(
            jnp.dot(
                table_parts,
                (kind_row == rows[3]).astype(jnp.float32).astype(jnp.bfloat16),
                preferred_element_type=jnp.float32,
            )
        )
        whole = jnp.concatenate(rows[0:3] + [found[0:3], rows[4], found[3:4]], axis=0)
        for q in range(blocks):
            params[place * blocks + q] = whole[:, q * LANES : (q + 1) * LANES]
        at = ROWS % per_row
        slots_here = ghost_ref[place, body + ROWS // per_row][:, at * 2 * mig : (at + 1) * 2 * mig]
        column = jnp.broadcast_to(slots_here, (8, 2 * mig)).T[:, 0:1]
        hot = jnp.broadcast_to(column, (2 * mig, atoms)) == atom_lane
        hot_ref[place] = hot.astype(jnp.float32).astype(jnp.bfloat16)

    def patch(a, b, c):
        place = slot((a, b, c))
        if isinstance(a, int) and a == 0:
            near, away = extra_rows(1, b, c), extra_rows(-1, b, c)
            pick = low_side > 0
        else:
            near, away = extra_rows(2 * a, b, c), extra_rows(0, b, c)
            pick = low_side * a > 0
        rows = [jnp.where(pick, x, y) for x, y in zip(near[:ROWS], away[:ROWS])]
        found = joined(
            jnp.dot(
                table_parts,
                (kind_row[:, : 2 * mig] == rows[3]).astype(jnp.float32).astype(jnp.bfloat16),
                preferred_element_type=jnp.float32,
            )
        )
        whole = jnp.concatenate(rows[0:3] + [found[0:3], rows[4], one_row], axis=0)
        spread = joined(
            jnp.dot(
                thirds(whole).astype(jnp.bfloat16),
                hot_ref[place],
                preferred_element_type=jnp.float32,
            )
        )
        for q in range(blocks):
            new = spread[:, q * LANES : (q + 1) * LANES]
            at = place * blocks + q
            params[at] = jnp.where(new[7:8] > 0.5, new, params[at])

    picks = (
        lax.broadcasted_iota(jnp.int32, (24, COLS * LANES), 0) % 8
        == lax.broadcasted_iota(jnp.int32, (24, COLS * LANES), 1) // LANES
    ).astype(jnp.float32).astype(jnp.bfloat16)

    def graded(flag):
        return [soft_base + (soft_alpha * lam) * flag, 1.0 - lam * flag]

    deep = lax.broadcasted_iota(jnp.int32, (8, LANES), 0)
    def own_side():
        for q in range(blocks):
            rows = params[own_slot * blocks + q]
            rows = jnp.concatenate([rows[0:5], rows[5:6] * (0.5 * coulomb), rows[6:8]], axis=0)
            cols = thirds(rows).T.astype(jnp.bfloat16)
            wide = jnp.dot(cols, picks, preferred_element_type=jnp.float32)
            for r in range(7):
                own_cols[q, r] = wide[:, r * LANES : (r + 1) * LANES]
            for r, col in enumerate(graded(own_cols[q, 6])):
                own_cols[q, 7 + r] = col
            flag = rows[6:7]
            (soft,) = graded(flag)[:1]
            ratio = 1.0 / soft
            root = lax.rsqrt(soft)
            plain = params[own_slot * blocks + q][5:6]
            electric = (coulomb * root) * plain * plain
            first = rows[4:5] * rows[4:5] * ratio
            second = first * ratio
            alone = second - first
            slope = (second + alone) * ratio + 0.5 * electric * (root * root)
            alone = alone + electric
            for k, value in enumerate((alone, flag * alone, flag * slope)):
                self_ref[q, k] = jnp.where(deep == 0, value, 0.0)

    for q in range(blocks):
        for k in range(3):
            force_acc[q, k] = jnp.zeros((LANES, LANES), jnp.float32)

    def arrive(a, b):
        here = slot((a, b, 0))
        passing(own, (a, b, 0), here, 0).wait_recv()
        for c in up:
            sends.append(passing(ghost_ref.at[here], (0, 0, -c), slot((a, b, c)), len(sends)))
            sends[-1].start()

    def across(a, b):
        for c in up:
            passing(own, (0, 0, -c), slot((a, b, c)), 0).wait_recv()
            prepare(a, b, c)

    nearest = sides[::-1]
    prepare(0, 0, 0)
    for b in nearest:
        if b:
            arrive(0, b)
            prepare(0, b, 0)
    across(0, 0)
    for a in reach[1:]:
        for b in nearest:
            arrive(a, b)
            prepare(a, b, 0)
    for b in nearest:
        if b:
            across(0, b)
    for a in reach[1:]:
        for b in nearest:
            across(a, b)
    for o in ends:
        far_copy(0, o, far_slot(*o)).wait_recv()
    for a in reach[1:]:
        for b in nearest:
            for c in steps_of(nz):
                patch(a, b, c)
    for a in reach[:1]:
        for b in nearest:
            arrive(a, b)
    for b in nearest:
        for a in reach[:1]:
            prepare(a, b, 0)
            patch(a, b, 0)
        patch(0, b, 0)
    own_side()
    for b in nearest:
        for a in reach[:1]:
            across(a, b)
        for c in up:
            for a in [0] + reach[:1]:
                patch(a, b, c)

    width = listed_ref.shape[-1]
    together = 2 if width % 2 == 0 else 1
    groups = 8 if width % (8 * together) == 0 else 1

    def listed_rows(q, e):
        listed = listed_ref[q, 0, e]
        image = lax.div(listed, blocks)
        a = lax.div(image, 9) - 1
        b = lax.rem(lax.div(image, 3), 3) - 1
        c = lax.rem(image, 3) - 1
        where_from = (
            slot_step(a, nx) * len(steps_of(ny)) + slot_step(b, ny)
        ) * len(steps_of(nz)) + slot_step(c, nz)
        other = params[where_from * blocks + lax.rem(listed, blocks)]
        return other, [x.astype(jnp.float32) * y for x, y in zip((a, b, c), edge)], listed

    def entry(q, e):
        other, step_by, listed = listed_rows(q, e)
        left = jnp.minimum(jnp.maximum(count_ref[0, 0, 0, q] - e, 0), 1)
        used = left.astype(jnp.float32)
        apart = jnp.abs(listed - (13 * blocks + q))
        itself = ((1 - jnp.minimum(apart, 1)) * left).astype(jnp.float32)
        rows = []
        for r in range(7):
            row = other[r : r + 1]
            if r < 3:
                row = row + step_by[r]
            if 4 <= r < 6:
                row = row * used
            rows.append(row)
        rows.append(graded(rows[6])[0])
        return [jnp.broadcast_to(row, (8, LANES)) for row in rows], itself

    @pl.loop(0, blocks)
    def _(q):
        def turn(step):
            others = [entry(q, step * together + k) for k in range(together)]
            tot, tot_p, tot_k = (
                sum(-itself * self_ref[q, k] for _, itself in others) for k in range(3)
            )
            for g in range(LANES // 8):
                at = pl.ds(g * 8, 8)
                xi, yi, zi, hi, ei, qi, pi, si = (own_cols[q, r, at] for r in range(8))
                for k, ((xj, yj, zj, hj, ej, qj, pj, sj), _) in enumerate(others):
                    dx, dy, dz = xi - xj, yi - yj, zi - zj
                    r2 = dx * dx + dy * dy + dz * dz
                    sig = hi + hj
                    s2 = sig * sig
                    s6 = s2 * s2 * s2
                    soft = jnp.maximum(si, sj)
                    p = jnp.maximum(pi, pj)
                    r4 = r2 * r2
                    inv = 1.0 / (s6 * soft + r4 * r2)
                    u = lax.rsqrt(3.0 * r2 + soft)
                    half = (qi * qj) * u
                    ec = half + half
                    half = half * (u * u)
                    t = s6 * inv
                    first = (ei * ej) * t
                    second = first * t
                    v = second - first
                    m = second + v
                    v = v + ec
                    kk = m * t + half
                    slopes[q, step * together + k, at] = m * (r4 * inv) + half
                    tot = tot + v
                    tot_p = tot_p + p * v
                    tot_k = tot_k + p * kk
            for k, value in enumerate((tot, tot_p, tot_k)):
                sums_ref[k] += value

        @pl.loop(0, width // (together * groups))
        def _(step):
            for k in range(groups):
                turn(step * groups + k)

    part = LANES // 4

    def narrowed(row):
        row = row + pltpu.roll(row, LANES // 2, 1)
        return row + pltpu.roll(row, part, 1)

    folded = [narrowed(jnp.sum(sums_ref[k], axis=0, keepdims=True)) for k in range(3)]
    lane = lax.broadcasted_iota(jnp.int32, (1, LANES), 1)
    mine = jnp.where(lane < part, folded[0], jnp.where(lane < 2 * part, folded[1], folded[2]))
    tile[...] = mine
    gathered[my_id] = mine

    def share(by):
        return pltpu.make_async_remote_copy(
            src_ref=tile,
            dst_ref=gathered.at[my_id],
            send_sem=sum_send.at[by],
            recv_sem=sum_recv.at[by],
            device_id=window_device(lax.rem(my_id + by, total)),
            device_id_type=MESH,
        )

    @pl.loop(1, total)
    def _(by):
        share(by).start()

    joint = 4 if width % 4 == 0 else 1

    @pl.loop(0, blocks)
    def _(q):
        def sweep(step):
            others = []
            for k in range(joint):
                other, step_by, _ = listed_rows(q, step * joint + k)
                rows = [other[r : r + 1] + step_by[r] for r in range(3)]
                rows.append(graded(other[6:7])[1])
                others.append([jnp.broadcast_to(row, (8, LANES)) for row in rows])
            for g in range(LANES // 8):
                at = pl.ds(g * 8, 8)
                xi, yi, zi, wi = (own_cols[q, r, at] for r in (0, 1, 2, 8))
                forces = None
                for k, (xj, yj, zj, wj) in enumerate(others):
                    fs = slopes[q, step * joint + k, at] * jnp.minimum(wi, wj)
                    new = [fs * (xi - xj), fs * (yi - yj), fs * (zi - zj)]
                    forces = new if forces is None else [x + y for x, y in zip(forces, new)]
                for k in range(3):
                    force_acc[q, k, at] += forces[k]

        for step in range(width // joint):
            sweep(step)

    for q in range(blocks):
        for k in range(3):
            whole = force_acc[q, k]
            high = whole.astype(jnp.bfloat16)
            low = (whole - high.astype(jnp.float32)).astype(jnp.bfloat16)
            reduced = sum(
                lax.dot_general(
                    ones, part, (((1,), (1,)), ((), ())), preferred_element_type=jnp.float32
                )
                for part in (high, low)
            )
            force_ref[k, 0, 0, :, q * LANES : (q + 1) * LANES] = (2.0 * 3.0**0.5) * reduced[0:1]

    for copy in sends + far_copies:
        copy.wait_send()

    @pl.loop(1, total)
    def _(by):
        share(by).wait()

    summed = jnp.sum(gathered[...], axis=0)
    parts = [
        jnp.sum(jnp.where(lax.div(lane, part) == k, summed, 0.0)) for k in range(3)
    ]
    scale = 0.5 / float(atoms * total)
    rows = lax.broadcasted_iota(jnp.int32, (8, LANES), 0)
    energy = scale * (parts[0] - lam * parts[1])
    dhdl = -scale * (parts[1] + (0.5 * (1.0 - lam)) * parts[2])
    tally_ref[...] = jnp.where(rows == 0, energy, dhdl)


def hand_over(force_in, tally_in, force_ref, energy_ref, dhdl_ref, sem):
    copy = pltpu.make_async_copy(force_in, force_ref, sem)
    copy.start()
    energy_ref[0] = tally_in[0, 0]
    dhdl_ref[0] = tally_in[1, 0]
    copy.wait()


def on_device(sizes, fraction, atom_type, perturbed, leaving, neighbours, counts,
              sigma_table, depth_table, charge_table, domain_edge, coupling):
    nx, ny, nz = sizes
    atoms = fraction.shape[-1]
    mig = leaving.shape[-1]
    slots = len(steps_of(nx)) * len(steps_of(ny)) * len(steps_of(nz))
    planar = len(steps_of(ny)) * len(steps_of(nz))
    far_slots = max(len(far_steps(nx)), 1) * planar
    extras = -(-(ROWS + 1) // (LANES // (2 * mig)))
    smem = pl.BlockSpec(memory_space=pltpu.SMEM)
    vmem = pl.BlockSpec(memory_space=pltpu.VMEM)
    f32 = jnp.float32

    def bound(kernel, *values):
        return lambda *refs: kernel(*values, *refs)

    blocks = atoms // LANES
    total = nx * ny * nz
    dma = pltpu.SemaphoreType.DMA
    arrays = (
        domain_edge,
        coupling,
        sigma_table,
        depth_table,
        charge_table,
        neighbours.reshape(blocks, 1, -1),
        counts,
        fraction,
        atom_type,
        perturbed,
        leaving,
    )
    forces, tally = pl.pallas_call(
        bound(step_kernel, sizes),
        name="step",
        out_shape=(pltpu.VMEM(fraction.shape, f32), pltpu.VMEM((8, LANES), f32)),
        in_specs=[pl.BlockSpec(memory_space=pl.ANY)] * 11,
        out_specs=(vmem, vmem),
        scratch_shapes=[
            *(pltpu.SMEM(x.shape, x.dtype) for x in arrays[:7]),
            *(pltpu.VMEM(x.shape, x.dtype) for x in arrays[7:]),
            dma((11,)),
            pltpu.VMEM((slots, blocks * ROWS + extras, 1, LANES), f32),
            pltpu.VMEM((far_slots, extras, 1, LANES), f32),
            pltpu.VMEM((slots, 2 * mig, atoms), jnp.bfloat16),
            pltpu.VMEM((blocks, COLS, LANES, LANES), f32),
            pltpu.VMEM((blocks, 3, LANES, LANES), f32),
            pltpu.VMEM((slots * blocks, 8, LANES), f32),
            pltpu.VMEM((blocks, 3, 8, LANES), f32),
            pltpu.VMEM((blocks, neighbours.shape[-1], LANES, LANES), f32),
            pltpu.VMEM((3, 8, LANES), f32),
            pltpu.VMEM((1, LANES), f32),
            pltpu.VMEM((total, 1, LANES), f32),
            dma((far_slots,)),
            dma((far_slots,)),
            dma((slots,)),
            dma((slots,)),
            dma((total,)),
            dma((total,)),
        ],
        compiler_params=pltpu.CompilerParams(collective_id=0, has_side_effects=True),
    )(*arrays)
    return pl.pallas_call(
        hand_over,
        name="hand_over",
        out_shape=(
            jax.ShapeDtypeStruct(fraction.shape, f32),
            jax.ShapeDtypeStruct((1,), f32),
            jax.ShapeDtypeStruct((1,), f32),
        ),
        in_specs=[vmem, vmem],
        out_specs=(pl.BlockSpec(memory_space=pl.ANY), smem, smem),
        scratch_shapes=[pltpu.SemaphoreType.DMA],
    )(pltpu.with_memory_space_constraint(forces, pltpu.VMEM), pltpu.with_memory_space_constraint(tally, pltpu.VMEM))


def solution(mesh):
    sizes = (mesh.shape["dx"], mesh.shape["dy"], mesh.shape["dz"])
    return jax.shard_map(
        lambda *arrays: on_device(sizes, *arrays),
        mesh=mesh,
        in_specs=(
            P(None, ("win", "dx"), "dy", "dz", None),
            P(("win", "dx"), "dy", "dz", None),
            P(("win", "dx"), "dy", "dz", None),
            P(("win", "dx"), "dy", "dz", None, None),
            P(("win", "dx"), "dy", "dz", None, None),
            P(("win", "dx"), "dy", "dz", None),
            P(),
            P(),
            P(),
            P(),
            P("win"),
        ),
        out_specs=(P(None, ("win", "dx"), "dy", "dz", None), P("win"), P("win")),
        check_vma=False,
    )
```

```python
import jax
import jax.numpy as jnp
from jax import lax
from jax.experimental import pallas as pl
from jax.experimental.pallas import tpu as pltpu
from jax.sharding import PartitionSpec as P

soft_base = 0.3
soft_alpha = 0.5
charge_base = 0.3
charge_alpha = 0.5
coulomb = 0.1
LANES = 128
MESH = pl.DeviceIdType.MESH
COLS = 9
ROWS = 5


def steps_of(count):
    return {1: (0,), 2: (0, 1)}.get(count, (-1, 0, 1))


def far_steps(count):
    return {1: (), 2: (), 3: (), 4: (2,)}.get(count, (2, -2))


def slot_step(step, count):
    if count == 1:
        return step * 0
    if count == 2:
        return step * step
    return step + 1


def thirds(value):
    high = value.astype(jnp.bfloat16).astype(jnp.float32)
    rest = value - high
    middle = rest.astype(jnp.bfloat16).astype(jnp.float32)
    return jnp.concatenate([high, middle, rest - middle], axis=0)


def joined(value):
    return value[0:8] + value[8:16] + value[16:24]


def step_kernel(
    sizes,
    *refs,
):
    inputs, refs = refs[:11], refs[11:]
    force_ref, tally_ref, *refs = refs
    staged, (load_sem, *refs) = refs[:11], refs[11:]
    (
        edge_ref,
        coupling_ref,
        sigma_ref,
        depth_ref,
        charge_ref,
        listed_ref,
        count_ref,
        fraction_ref,
        type_ref,
        flag_ref,
        leaving_ref,
    ) = staged
    (
        ghost_ref,
        far_ref,
        hot_ref,
        own_cols,
        force_acc,
        params,
        self_ref,
        slopes,
        sums_ref,
        tile,
        gathered,
        far_send,
        far_recv,
        send_sem,
        recv_sem,
        sum_send,
        sum_recv,
    ) = refs
    nx, ny, nz = sizes
    atoms = fraction_ref.shape[-1]
    spacing = float(atoms) ** (1.0 / 3.0)
    me = (lax.axis_index("dx"), lax.axis_index("dy"), lax.axis_index("dz"))

    def device(step):
        return {
            name: lax.rem(place + by + count, count)
            for name, place, by, count in zip(("dx", "dy", "dz"), me, step, sizes)
        }

    offsets = [(a, b, c) for a in steps_of(nx) for b in steps_of(ny) for c in steps_of(nz)]
    others = [o for o in offsets if any(o)]

    def slot(o):
        return (
            slot_step(o[0], nx) * len(steps_of(ny)) + slot_step(o[1], ny)
        ) * len(steps_of(nz)) + slot_step(o[2], nz)

    barrier = pltpu.get_barrier_semaphore()
    total = nx * ny * nz
    my_id = (me[0] * ny + me[1]) * nz + me[2]

    def window_device(k):
        return {
            "dx": lax.div(k, ny * nz),
            "dy": lax.rem(lax.div(k, nz), ny),
            "dz": lax.rem(k, nz),
        }

    @pl.loop(1, total)
    def _(by):
        pl.semaphore_signal(
            barrier,
            inc=1,
            device_id=window_device(lax.rem(my_id + by, total)),
            device_id_type=MESH,
        )

    loads = [
        pltpu.make_async_copy(source, target, load_sem.at[k])
        for k, (source, target) in enumerate(zip(inputs, staged))
    ]
    for load in loads:
        load.start()
    for load in loads:
        load.wait()

    own = ghost_ref.at[slot((0, 0, 0))]
    edge = [edge_ref[k] * (spacing * 3.0**-0.5) for k in range(3)]
    rows = [fraction_ref[k, 0, 0] * edge[k] for k in range(3)]
    rows += [type_ref[0, 0].astype(jnp.float32), flag_ref[0, 0].astype(jnp.float32)]
    payload = jnp.concatenate(rows + [jnp.zeros((3, atoms), jnp.float32)], axis=0)
    leave = leaving_ref[0, 0, 0]
    mig = leave.shape[1]
    slots_in = jnp.concatenate([leave[0:1], leave[1:2]], axis=1)
    slots_out = jnp.concatenate([leave[1:2], leave[0:1]], axis=1)
    place = lax.broadcasted_iota(jnp.int32, (atoms, 2 * mig), 0)
    hot_out = (place == slots_out).astype(jnp.float32).astype(jnp.bfloat16)
    lane = lax.broadcasted_iota(jnp.int32, (8, 2 * mig), 1)
    deep = lax.broadcasted_iota(jnp.int32, (8, 2 * mig), 0)
    shift = jnp.where(deep == 0, jnp.where(lane < mig, edge[0], -edge[0]), 0.0)
    leavers = joined(
        jnp.dot(thirds(payload).astype(jnp.bfloat16), hot_out, preferred_element_type=jnp.float32)
    )
    leavers = leavers + shift
    blocks = atoms // LANES
    body = blocks * ROWS
    per_row = LANES // (2 * mig)
    extras = -(-(ROWS + 1) // per_row)
    for q in range(blocks):
        for r in range(ROWS):
            own[q * ROWS + r] = payload[r : r + 1, q * LANES : (q + 1) * LANES]
    parts = [leavers[r : r + 1] for r in range(ROWS)] + [slots_in.astype(jnp.float32)]
    parts += [parts[0] * 0.0] * (extras * per_row - ROWS - 1)
    for r in range(extras):
        own[body + r] = jnp.concatenate(parts[r * per_row : (r + 1) * per_row], axis=1)

    pl.semaphore_wait(barrier, total - 1)

    def passing(source, target, place, k):
        return pltpu.make_async_remote_copy(
            src_ref=source,
            dst_ref=ghost_ref.at[place],
            send_sem=send_sem.at[k],
            recv_sem=recv_sem.at[place],
            device_id=device(target),
            device_id_type=MESH,
        )

    fars = far_steps(nx)
    ends = [(a, b, c) for a in fars for b in steps_of(ny) for c in steps_of(nz)]

    def far_slot(a, b, c):
        which = (2 - a) // 4 if len(fars) > 1 else 0
        return (which * len(steps_of(ny)) + slot_step(b, ny)) * len(steps_of(nz)) + slot_step(c, nz)

    def far_copy(k, target, here):
        return pltpu.make_async_remote_copy(
            src_ref=own.at[pl.ds(body, extras)],
            dst_ref=far_ref.at[here],
            send_sem=far_send.at[k],
            recv_sem=far_recv.at[here],
            device_id=device(target),
            device_id_type=MESH,
        )

    far_copies = [
        far_copy(k, (a, b, c), far_slot(-a if len(fars) > 1 else a, -b, -c))
        for k, (a, b, c) in enumerate(ends)
    ]
    for copy in far_copies:
        copy.start()

    if nx > 2:
        toward = 2 * lax.div(2 * me[0], nx) - 1
        reach = [toward, -toward]
    else:
        reach = [x for x in steps_of(nx) if x]
    sides = sorted((b for b in steps_of(ny)), key=lambda b: -abs(b))
    plan = [(a, b) for a in reach for b in sides] + [(0, b) for b in sides if b]
    up = [c for c in steps_of(nz) if c]
    sends = []
    for a, b in plan:
        sends.append(passing(own, (a, b, 0), slot((-a, -b, 0)), len(sends)))
        sends[-1].start()
    for c in up:
        sends.append(passing(own, (0, 0, -c), slot((0, 0, c)), len(sends)))
        sends[-1].start()

    lam = coupling_ref[0]
    own_slot = slot((0, 0, 0))
    ones = jnp.ones((8, LANES), jnp.bfloat16)
    for k in range(3):
        sums_ref[k] = jnp.zeros((8, LANES), jnp.float32)

    lane = lax.broadcasted_iota(jnp.int32, (1, LANES), 1)
    tables = [jnp.zeros((1, LANES), jnp.float32)] * 3
    for k in range(sigma_ref.shape[0]):
        hit = lane == k
        tables = [
            jnp.where(hit, ref[k], table)
            for ref, table in zip((sigma_ref, depth_ref, charge_ref), tables)
        ]
    table = jnp.concatenate(
        [tables[0] * (0.5 * 3.0**-0.5), jnp.sqrt(tables[1]) * 2.0, tables[2]]
        + [tables[2] * 0.0] * 5,
        axis=0,
    )
    kinds = sigma_ref.shape[0]
    table_parts = thirds(table[:, :kinds]).astype(jnp.bfloat16)
    kind_row = lax.broadcasted_iota(jnp.int32, (kinds, atoms), 0).astype(jnp.float32)

    low_side = jnp.where(lax.broadcasted_iota(jnp.int32, (1, 2 * mig), 1) < mig, 1, -1)
    atom_lane = lax.broadcasted_iota(jnp.int32, (2 * mig, atoms), 1).astype(jnp.float32)
    one_row = jnp.ones((1, 2 * mig), jnp.float32)

    def extra_rows(a, b, c):
        far = not isinstance(a, int) or abs(a) == 2
        if far and fars:
            found = [far_ref[far_slot(a, b, c), r] for r in range(extras)]
        else:
            if far:
                a = -a // 2 if nx == 3 else 0
            found = [ghost_ref[slot((a, b, c)), body + r] for r in range(extras)]
        return [
            found[r // per_row][:, (r % per_row) * 2 * mig : (r % per_row + 1) * 2 * mig]
            for r in range(ROWS + 1)
        ]

    def prepare(a, b, c):
        place = slot((a, b, c))
        rows = [
            jnp.concatenate([ghost_ref[place, q * ROWS + r] for q in range(blocks)], axis=1)
            for r in range(ROWS)
        ]
        found = joined(
            jnp.dot(
                table_parts,
                (kind_row == rows[3]).astype(jnp.float32).astype(jnp.bfloat16),
                preferred_element_type=jnp.float32,
            )
        )
        whole = jnp.concatenate(rows[0:3] + [found[0:3], rows[4], found[3:4]], axis=0)
        for q in range(blocks):
            params[place * blocks + q] = whole[:, q * LANES : (q + 1) * LANES]
        at = ROWS % per_row
        slots_here = ghost_ref[place, body + ROWS // per_row][:, at * 2 * mig : (at + 1) * 2 * mig]
        column = jnp.broadcast_to(slots_here, (8, 2 * mig)).T[:, 0:1]
        hot = jnp.broadcast_to(column, (2 * mig, atoms)) == atom_lane
        hot_ref[place] = hot.astype(jnp.float32).astype(jnp.bfloat16)

    def patch(a, b, c):
        place = slot((a, b, c))
        if isinstance(a, int) and a == 0:
            near, away = extra_rows(1, b, c), extra_rows(-1, b, c)
            pick = low_side > 0
        else:
            near, away = extra_rows(2 * a, b, c), extra_rows(0, b, c)
            pick = low_side * a > 0
        rows = [jnp.where(pick, x, y) for x, y in zip(near[:ROWS], away[:ROWS])]
        found = joined(
            jnp.dot(
                table_parts,
                (kind_row[:, : 2 * mig] == rows[3]).astype(jnp.float32).astype(jnp.bfloat16),
                preferred_element_type=jnp.float32,
            )
        )
        whole = jnp.concatenate(rows[0:3] + [found[0:3], rows[4], one_row], axis=0)
        spread = joined(
            jnp.dot(
                thirds(whole).astype(jnp.bfloat16),
                hot_ref[place],
                preferred_element_type=jnp.float32,
            )
        )
        for q in range(blocks):
            new = spread[:, q * LANES : (q + 1) * LANES]
            at = place * blocks + q
            params[at] = jnp.where(new[7:8] > 0.5, new, params[at])

    picks = (
        lax.broadcasted_iota(jnp.int32, (24, COLS * LANES), 0) % 8
        == lax.broadcasted_iota(jnp.int32, (24, COLS * LANES), 1) // LANES
    ).astype(jnp.float32).astype(jnp.bfloat16)

    def graded(flag):
        return [soft_base + (soft_alpha * lam) * flag, 1.0 - lam * flag]

    deep = lax.broadcasted_iota(jnp.int32, (8, LANES), 0)
    def own_side():
        for q in range(blocks):
            rows = params[own_slot * blocks + q]
            rows = jnp.concatenate([rows[0:5], rows[5:6] * (0.5 * coulomb), rows[6:8]], axis=0)
            cols = thirds(rows).T.astype(jnp.bfloat16)
            wide = jnp.dot(cols, picks, preferred_element_type=jnp.float32)
            for r in range(7):
                own_cols[q, r] = wide[:, r * LANES : (r + 1) * LANES]
            for r, col in enumerate(graded(own_cols[q, 6])):
                own_cols[q, 7 + r] = col
            flag = rows[6:7]
            (soft,) = graded(flag)[:1]
            ratio = 1.0 / soft
            root = lax.rsqrt(soft)
            plain = params[own_slot * blocks + q][5:6]
            electric = (coulomb * root) * plain * plain
            first = rows[4:5] * rows[4:5] * ratio
            second = first * ratio
            alone = second - first
            slope = (second + alone) * ratio + 0.5 * electric * (root * root)
            alone = alone + electric
            for k, value in enumerate((alone, flag * alone, flag * slope)):
                self_ref[q, k] = jnp.where(deep == 0, value, 0.0)

    for q in range(blocks):
        for k in range(3):
            force_acc[q, k] = jnp.zeros((LANES, LANES), jnp.float32)

    def arrive(a, b):
        here = slot((a, b, 0))
        passing(own, (a, b, 0), here, 0).wait_recv()
        for c in up:
            sends.append(passing(ghost_ref.at[here], (0, 0, -c), slot((a, b, c)), len(sends)))
            sends[-1].start()

    def across(a, b):
        for c in up:
            passing(own, (0, 0, -c), slot((a, b, c)), 0).wait_recv()
            prepare(a, b, c)

    nearest = sides[::-1]
    prepare(0, 0, 0)
    for b in nearest:
        if b:
            arrive(0, b)
            prepare(0, b, 0)
    across(0, 0)
    for a in reach[1:]:
        for b in nearest:
            arrive(a, b)
            prepare(a, b, 0)
    for b in nearest:
        if b:
            across(0, b)
    for a in reach[1:]:
        for b in nearest:
            across(a, b)
    for o in ends:
        far_copy(0, o, far_slot(*o)).wait_recv()
    for a in reach[1:]:
        for b in nearest:
            for c in steps_of(nz):
                patch(a, b, c)
    for a in reach[:1]:
        for b in nearest:
            arrive(a, b)
    for b in nearest:
        for a in reach[:1]:
            prepare(a, b, 0)
            patch(a, b, 0)
        patch(0, b, 0)
    own_side()
    for b in nearest:
        for a in reach[:1]:
            across(a, b)
        for c in up:
            for a in [0] + reach[:1]:
                patch(a, b, c)

    width = listed_ref.shape[-1]
    together = 1 if width % 1 == 0 else 1
    groups = 16 if width % (16 * together) == 0 else 1

    def listed_rows(q, e):
        listed = listed_ref[q, 0, e]
        image = lax.div(listed, blocks)
        a = lax.div(image, 9) - 1
        b = lax.rem(lax.div(image, 3), 3) - 1
        c = lax.rem(image, 3) - 1
        where_from = (
            slot_step(a, nx) * len(steps_of(ny)) + slot_step(b, ny)
        ) * len(steps_of(nz)) + slot_step(c, nz)
        other = params[where_from * blocks + lax.rem(listed, blocks)]
        return other, [x.astype(jnp.float32) * y for x, y in zip((a, b, c), edge)], listed

    def entry(q, e):
        other, step_by, listed = listed_rows(q, e)
        left = jnp.minimum(jnp.maximum(count_ref[0, 0, 0, q] - e, 0), 1)
        used = left.astype(jnp.float32)
        apart = jnp.abs(listed - (13 * blocks + q))
        itself = ((1 - jnp.minimum(apart, 1)) * left).astype(jnp.float32)
        rows = []
        for r in range(7):
            row = other[r : r + 1]
            if r < 3:
                row = row + step_by[r]
            if 4 <= r < 6:
                row = row * used
            rows.append(row)
        rows.append(graded(rows[6])[0])
        return [jnp.broadcast_to(row, (8, LANES)) for row in rows], itself

    @pl.loop(0, blocks)
    def _(q):
        def turn(step):
            others = [entry(q, step * together + k) for k in range(together)]
            tot, tot_p, tot_k = (
                sum(-itself * self_ref[q, k] for _, itself in others) for k in range(3)
            )
            for g in range(LANES // 8):
                at = pl.ds(g * 8, 8)
                xi, yi, zi, hi, ei, qi, pi, si = (own_cols[q, r, at] for r in range(8))
                for k, ((xj, yj, zj, hj, ej, qj, pj, sj), _) in enumerate(others):
                    dx, dy, dz = xi - xj, yi - yj, zi - zj
                    r2 = dx * dx + dy * dy + dz * dz
                    sig = hi + hj
                    is2 = 1.0 / (sig * sig)
                    soft = jnp.maximum(si, sj)
                    p = jnp.maximum(pi, pj)
                    x = r2 * is2
                    x2 = x * x
                    t = 1.0 / (soft + x2 * x)
                    u = lax.rsqrt(3.0 * r2 + soft)
                    half = (qi * qj) * u
                    ec = half + half
                    half = half * (u * u)
                    first = (ei * ej) * t
                    second = first * t
                    v = second - first
                    mt = (second + v) * t
                    v = v + ec
                    kk = mt + half
                    slopes[q, step * together + k, at] = mt * (x2 * is2) + half
                    tot = tot + v
                    tot_p = tot_p + p * v
                    tot_k = tot_k + p * kk
            for k, value in enumerate((tot, tot_p, tot_k)):
                sums_ref[k] += value

        @pl.loop(0, width // (together * groups))
        def _(step):
            for k in range(groups):
                turn(step * groups + k)

    part = LANES // 4

    def narrowed(row):
        row = row + pltpu.roll(row, LANES // 2, 1)
        return row + pltpu.roll(row, part, 1)

    folded = [narrowed(jnp.sum(sums_ref[k], axis=0, keepdims=True)) for k in range(3)]
    lane = lax.broadcasted_iota(jnp.int32, (1, LANES), 1)
    mine = jnp.where(lane < part, folded[0], jnp.where(lane < 2 * part, folded[1], folded[2]))
    tile[...] = mine
    gathered[my_id] = mine

    def share(by):
        return pltpu.make_async_remote_copy(
            src_ref=tile,
            dst_ref=gathered.at[my_id],
            send_sem=sum_send.at[by],
            recv_sem=sum_recv.at[by],
            device_id=window_device(lax.rem(my_id + by, total)),
            device_id_type=MESH,
        )

    @pl.loop(1, total)
    def _(by):
        share(by).start()

    joint = 4 if width % 4 == 0 else 1

    @pl.loop(0, blocks)
    def _(q):
        def sweep(step):
            others = []
            for k in range(joint):
                other, step_by, _ = listed_rows(q, step * joint + k)
                rows = [other[r : r + 1] + step_by[r] for r in range(3)]
                rows.append(graded(other[6:7])[1])
                others.append([jnp.broadcast_to(row, (8, LANES)) for row in rows])
            for g in range(LANES // 8):
                at = pl.ds(g * 8, 8)
                xi, yi, zi, wi = (own_cols[q, r, at] for r in (0, 1, 2, 8))
                forces = None
                for k, (xj, yj, zj, wj) in enumerate(others):
                    fs = slopes[q, step * joint + k, at] * jnp.minimum(wi, wj)
                    new = [fs * (xi - xj), fs * (yi - yj), fs * (zi - zj)]
                    forces = new if forces is None else [x + y for x, y in zip(forces, new)]
                for k in range(3):
                    force_acc[q, k, at] += forces[k]

        for step in range(width // joint):
            sweep(step)

    for q in range(blocks):
        for k in range(3):
            whole = force_acc[q, k]
            high = whole.astype(jnp.bfloat16)
            low = (whole - high.astype(jnp.float32)).astype(jnp.bfloat16)
            reduced = sum(
                lax.dot_general(
                    ones, part, (((1,), (1,)), ((), ())), preferred_element_type=jnp.float32
                )
                for part in (high, low)
            )
            force_ref[k, 0, 0, :, q * LANES : (q + 1) * LANES] = (2.0 * 3.0**0.5) * reduced[0:1]

    for copy in sends + far_copies:
        copy.wait_send()

    @pl.loop(1, total)
    def _(by):
        share(by).wait()

    summed = jnp.sum(gathered[...], axis=0)
    parts = [
        jnp.sum(jnp.where(lax.div(lane, part) == k, summed, 0.0)) for k in range(3)
    ]
    scale = 0.5 / float(atoms * total)
    rows = lax.broadcasted_iota(jnp.int32, (8, LANES), 0)
    energy = scale * (parts[0] - lam * parts[1])
    dhdl = -scale * (parts[1] + (0.5 * (1.0 - lam)) * parts[2])
    tally_ref[...] = jnp.where(rows == 0, energy, dhdl)


def hand_over(force_in, tally_in, force_ref, energy_ref, dhdl_ref, sem):
    copy = pltpu.make_async_copy(force_in, force_ref, sem)
    copy.start()
    energy_ref[0] = tally_in[0, 0]
    dhdl_ref[0] = tally_in[1, 0]
    copy.wait()


def on_device(sizes, fraction, atom_type, perturbed, leaving, neighbours, counts,
              sigma_table, depth_table, charge_table, domain_edge, coupling):
    nx, ny, nz = sizes
    atoms = fraction.shape[-1]
    mig = leaving.shape[-1]
    slots = len(steps_of(nx)) * len(steps_of(ny)) * len(steps_of(nz))
    planar = len(steps_of(ny)) * len(steps_of(nz))
    far_slots = max(len(far_steps(nx)), 1) * planar
    extras = -(-(ROWS + 1) // (LANES // (2 * mig)))
    smem = pl.BlockSpec(memory_space=pltpu.SMEM)
    vmem = pl.BlockSpec(memory_space=pltpu.VMEM)
    f32 = jnp.float32

    def bound(kernel, *values):
        return lambda *refs: kernel(*values, *refs)

    blocks = atoms // LANES
    total = nx * ny * nz
    dma = pltpu.SemaphoreType.DMA
    arrays = (
        domain_edge,
        coupling,
        sigma_table,
        depth_table,
        charge_table,
        neighbours.reshape(blocks, 1, -1),
        counts,
        fraction,
        atom_type,
        perturbed,
        leaving,
    )
    forces, tally = pl.pallas_call(
        bound(step_kernel, sizes),
        name="step",
        out_shape=(pltpu.VMEM(fraction.shape, f32), pltpu.VMEM((8, LANES), f32)),
        in_specs=[pl.BlockSpec(memory_space=pl.ANY)] * 11,
        out_specs=(vmem, vmem),
        scratch_shapes=[
            *(pltpu.SMEM(x.shape, x.dtype) for x in arrays[:7]),
            *(pltpu.VMEM(x.shape, x.dtype) for x in arrays[7:]),
            dma((11,)),
            pltpu.VMEM((slots, blocks * ROWS + extras, 1, LANES), f32),
            pltpu.VMEM((far_slots, extras, 1, LANES), f32),
            pltpu.VMEM((slots, 2 * mig, atoms), jnp.bfloat16),
            pltpu.VMEM((blocks, COLS, LANES, LANES), f32),
            pltpu.VMEM((blocks, 3, LANES, LANES), f32),
            pltpu.VMEM((slots * blocks, 8, LANES), f32),
            pltpu.VMEM((blocks, 3, 8, LANES), f32),
            pltpu.VMEM((blocks, neighbours.shape[-1], LANES, LANES), f32),
            pltpu.VMEM((3, 8, LANES), f32),
            pltpu.VMEM((1, LANES), f32),
            pltpu.VMEM((total, 1, LANES), f32),
            dma((far_slots,)),
            dma((far_slots,)),
            dma((slots,)),
            dma((slots,)),
            dma((total,)),
            dma((total,)),
        ],
        compiler_params=pltpu.CompilerParams(collective_id=0, has_side_effects=True),
    )(*arrays)
    return pl.pallas_call(
        hand_over,
        name="hand_over",
        out_shape=(
            jax.ShapeDtypeStruct(fraction.shape, f32),
            jax.ShapeDtypeStruct((1,), f32),
            jax.ShapeDtypeStruct((1,), f32),
        ),
        in_specs=[vmem, vmem],
        out_specs=(pl.BlockSpec(memory_space=pl.ANY), smem, smem),
        scratch_shapes=[pltpu.SemaphoreType.DMA],
    )(pltpu.with_memory_space_constraint(forces, pltpu.VMEM), pltpu.with_memory_space_constraint(tally, pltpu.VMEM))


def solution(mesh):
    sizes = (mesh.shape["dx"], mesh.shape["dy"], mesh.shape["dz"])
    return jax.shard_map(
        lambda *arrays: on_device(sizes, *arrays),
        mesh=mesh,
        in_specs=(
            P(None, ("win", "dx"), "dy", "dz", None),
            P(("win", "dx"), "dy", "dz", None),
            P(("win", "dx"), "dy", "dz", None),
            P(("win", "dx"), "dy", "dz", None, None),
            P(("win", "dx"), "dy", "dz", None, None),
            P(("win", "dx"), "dy", "dz", None),
            P(),
            P(),
            P(),
            P(),
            P("win"),
        ),
        out_specs=(P(None, ("win", "dx"), "dy", "dz", None), P("win"), P("win")),
        check_vma=False,
    )
```

```python
import jax
import jax.numpy as jnp
from jax import lax
from jax.experimental import pallas as pl
from jax.experimental.pallas import tpu as pltpu
from jax.sharding import PartitionSpec as P

soft_base = 0.3
soft_alpha = 0.5
charge_base = 0.3
charge_alpha = 0.5
coulomb = 0.1
LANES = 128
MESH = pl.DeviceIdType.MESH
COLS = 9
ROWS = 5


def steps_of(count):
    return {1: (0,), 2: (0, 1)}.get(count, (-1, 0, 1))


def far_steps(count):
    return {1: (), 2: (), 3: (), 4: (2,)}.get(count, (2, -2))


def slot_step(step, count):
    if count == 1:
        return step * 0
    if count == 2:
        return step * step
    return step + 1


def thirds(value):
    high = value.astype(jnp.bfloat16).astype(jnp.float32)
    rest = value - high
    middle = rest.astype(jnp.bfloat16).astype(jnp.float32)
    return jnp.concatenate([high, middle, rest - middle], axis=0)


def joined(value):
    return value[0:8] + value[8:16] + value[16:24]


def step_kernel(
    sizes,
    *refs,
):
    inputs, refs = refs[:11], refs[11:]
    force_ref, tally_ref, *refs = refs
    staged, (load_sem, *refs) = refs[:11], refs[11:]
    (
        edge_ref,
        coupling_ref,
        sigma_ref,
        depth_ref,
        charge_ref,
        listed_ref,
        count_ref,
        fraction_ref,
        type_ref,
        flag_ref,
        leaving_ref,
    ) = staged
    (
        ghost_ref,
        far_ref,
        hot_ref,
        own_cols,
        force_acc,
        params,
        self_ref,
        slopes,
        sums_ref,
        tile,
        gathered,
        far_send,
        far_recv,
        send_sem,
        recv_sem,
        sum_send,
        sum_recv,
    ) = refs
    nx, ny, nz = sizes
    atoms = fraction_ref.shape[-1]
    spacing = float(atoms) ** (1.0 / 3.0)
    me = (lax.axis_index("dx"), lax.axis_index("dy"), lax.axis_index("dz"))

    def device(step):
        return {
            name: lax.rem(place + by + count, count)
            for name, place, by, count in zip(("dx", "dy", "dz"), me, step, sizes)
        }

    offsets = [(a, b, c) for a in steps_of(nx) for b in steps_of(ny) for c in steps_of(nz)]
    others = [o for o in offsets if any(o)]

    def slot(o):
        return (
            slot_step(o[0], nx) * len(steps_of(ny)) + slot_step(o[1], ny)
        ) * len(steps_of(nz)) + slot_step(o[2], nz)

    barrier = pltpu.get_barrier_semaphore()
    total = nx * ny * nz
    my_id = (me[0] * ny + me[1]) * nz + me[2]

    def window_device(k):
        return {
            "dx": lax.div(k, ny * nz),
            "dy": lax.rem(lax.div(k, nz), ny),
            "dz": lax.rem(k, nz),
        }

    @pl.loop(1, total)
    def _(by):
        pl.semaphore_signal(
            barrier,
            inc=1,
            device_id=window_device(lax.rem(my_id + by, total)),
            device_id_type=MESH,
        )

    loads = [
        pltpu.make_async_copy(source, target, load_sem.at[k])
        for k, (source, target) in enumerate(zip(inputs, staged))
    ]
    for load in loads:
        load.start()
    for load in loads:
        load.wait()

    own = ghost_ref.at[slot((0, 0, 0))]
    edge = [edge_ref[k] * (spacing * 3.0**-0.5) for k in range(3)]
    rows = [fraction_ref[k, 0, 0] * edge[k] for k in range(3)]
    rows += [type_ref[0, 0].astype(jnp.float32), flag_ref[0, 0].astype(jnp.float32)]
    payload = jnp.concatenate(rows + [jnp.zeros((3, atoms), jnp.float32)], axis=0)
    leave = leaving_ref[0, 0, 0]
    mig = leave.shape[1]
    slots_in = jnp.concatenate([leave[0:1], leave[1:2]], axis=1)
    slots_out = jnp.concatenate([leave[1:2], leave[0:1]], axis=1)
    place = lax.broadcasted_iota(jnp.int32, (atoms, 2 * mig), 0)
    hot_out = (place == slots_out).astype(jnp.float32).astype(jnp.bfloat16)
    lane = lax.broadcasted_iota(jnp.int32, (8, 2 * mig), 1)
    deep = lax.broadcasted_iota(jnp.int32, (8, 2 * mig), 0)
    shift = jnp.where(deep == 0, jnp.where(lane < mig, edge[0], -edge[0]), 0.0)
    leavers = joined(
        jnp.dot(thirds(payload).astype(jnp.bfloat16), hot_out, preferred_element_type=jnp.float32)
    )
    leavers = leavers + shift
    blocks = atoms // LANES
    body = blocks * ROWS
    per_row = LANES // (2 * mig)
    extras = -(-(ROWS + 1) // per_row)
    for q in range(blocks):
        for r in range(ROWS):
            own[q * ROWS + r] = payload[r : r + 1, q * LANES : (q + 1) * LANES]
    parts = [leavers[r : r + 1] for r in range(ROWS)] + [slots_in.astype(jnp.float32)]
    parts += [parts[0] * 0.0] * (extras * per_row - ROWS - 1)
    for r in range(extras):
        own[body + r] = jnp.concatenate(parts[r * per_row : (r + 1) * per_row], axis=1)

    pl.semaphore_wait(barrier, total - 1)

    def passing(source, target, place, k):
        return pltpu.make_async_remote_copy(
            src_ref=source,
            dst_ref=ghost_ref.at[place],
            send_sem=send_sem.at[k],
            recv_sem=recv_sem.at[place],
            device_id=device(target),
            device_id_type=MESH,
        )

    fars = far_steps(nx)
    ends = [(a, b, c) for a in fars for b in steps_of(ny) for c in steps_of(nz)]

    def far_slot(a, b, c):
        which = (2 - a) // 4 if len(fars) > 1 else 0
        return (which * len(steps_of(ny)) + slot_step(b, ny)) * len(steps_of(nz)) + slot_step(c, nz)

    def far_copy(k, target, here):
        return pltpu.make_async_remote_copy(
            src_ref=own.at[pl.ds(body, extras)],
            dst_ref=far_ref.at[here],
            send_sem=far_send.at[k],
            recv_sem=far_recv.at[here],
            device_id=device(target),
            device_id_type=MESH,
        )

    far_copies = [
        far_copy(k, (a, b, c), far_slot(-a if len(fars) > 1 else a, -b, -c))
        for k, (a, b, c) in enumerate(ends)
    ]
    for copy in far_copies:
        copy.start()

    if nx > 2:
        toward = 2 * lax.div(2 * me[0], nx) - 1
        reach = [toward, -toward]
    else:
        reach = [x for x in steps_of(nx) if x]
    sides = sorted((b for b in steps_of(ny)), key=lambda b: -abs(b))
    plan = [(a, b) for a in reach for b in sides] + [(0, b) for b in sides if b]
    up = [c for c in steps_of(nz) if c]
    sends = []
    for a, b in plan:
        sends.append(passing(own, (a, b, 0), slot((-a, -b, 0)), len(sends)))
        sends[-1].start()
    for c in up:
        sends.append(passing(own, (0, 0, -c), slot((0, 0, c)), len(sends)))
        sends[-1].start()

    lam = coupling_ref[0]
    own_slot = slot((0, 0, 0))
    ones = jnp.ones((8, LANES), jnp.bfloat16)
    for k in range(3):
        sums_ref[k] = jnp.zeros((8, LANES), jnp.float32)

    lane = lax.broadcasted_iota(jnp.int32, (1, LANES), 1)
    tables = [jnp.zeros((1, LANES), jnp.float32)] * 3
    for k in range(sigma_ref.shape[0]):
        hit = lane == k
        tables = [
            jnp.where(hit, ref[k], table)
            for ref, table in zip((sigma_ref, depth_ref, charge_ref), tables)
        ]
    table = jnp.concatenate(
        [tables[0] * (0.5 * 3.0**-0.5), jnp.sqrt(tables[1]) * 2.0, tables[2]]
        + [tables[2] * 0.0] * 5,
        axis=0,
    )
    kinds = sigma_ref.shape[0]
    table_parts = thirds(table[:, :kinds]).astype(jnp.bfloat16)
    kind_row = lax.broadcasted_iota(jnp.int32, (kinds, atoms), 0).astype(jnp.float32)

    low_side = jnp.where(lax.broadcasted_iota(jnp.int32, (1, 2 * mig), 1) < mig, 1, -1)
    atom_lane = lax.broadcasted_iota(jnp.int32, (2 * mig, atoms), 1).astype(jnp.float32)
    one_row = jnp.ones((1, 2 * mig), jnp.float32)

    def extra_rows(a, b, c):
        far = not isinstance(a, int) or abs(a) == 2
        if far and fars:
            found = [far_ref[far_slot(a, b, c), r] for r in range(extras)]
        else:
            if far:
                a = -a // 2 if nx == 3 else 0
            found = [ghost_ref[slot((a, b, c)), body + r] for r in range(extras)]
        return [
            found[r // per_row][:, (r % per_row) * 2 * mig : (r % per_row + 1) * 2 * mig]
            for r in range(ROWS + 1)
        ]

    def prepare(a, b, c):
        place = slot((a, b, c))
        rows = [
            jnp.concatenate([ghost_ref[place, q * ROWS + r] for q in range(blocks)], axis=1)
            for r in range(ROWS)
        ]
        found = joined(
            jnp.dot(
                table_parts,
                (kind_row == rows[3]).astype(jnp.float32).astype(jnp.bfloat16),
                preferred_element_type=jnp.float32,
            )
        )
        whole = jnp.concatenate(rows[0:3] + [found[0:3], rows[4], found[3:4]], axis=0)
        for q in range(blocks):
            params[place * blocks + q] = whole[:, q * LANES : (q + 1) * LANES]
        at = ROWS % per_row
        slots_here = ghost_ref[place, body + ROWS // per_row][:, at * 2 * mig : (at + 1) * 2 * mig]
        column = jnp.broadcast_to(slots_here, (8, 2 * mig)).T[:, 0:1]
        hot = jnp.broadcast_to(column, (2 * mig, atoms)) == atom_lane
        hot_ref[place] = hot.astype(jnp.float32).astype(jnp.bfloat16)

    def patch(a, b, c):
        place = slot((a, b, c))
        if isinstance(a, int) and a == 0:
            near, away = extra_rows(1, b, c), extra_rows(-1, b, c)
            pick = low_side > 0
        else:
            near, away = extra_rows(2 * a, b, c), extra_rows(0, b, c)
            pick = low_side * a > 0
        rows = [jnp.where(pick, x, y) for x, y in zip(near[:ROWS], away[:ROWS])]
        found = joined(
            jnp.dot(
                table_parts,
                (kind_row[:, : 2 * mig] == rows[3]).astype(jnp.float32).astype(jnp.bfloat16),
                preferred_element_type=jnp.float32,
            )
        )
        whole = jnp.concatenate(rows[0:3] + [found[0:3], rows[4], one_row], axis=0)
        spread = joined(
            jnp.dot(
                thirds(whole).astype(jnp.bfloat16),
                hot_ref[place],
                preferred_element_type=jnp.float32,
            )
        )
        for q in range(blocks):
            new = spread[:, q * LANES : (q + 1) * LANES]
            at = place * blocks + q
            params[at] = jnp.where(new[7:8] > 0.5, new, params[at])

    picks = (
        lax.broadcasted_iota(jnp.int32, (24, COLS * LANES), 0) % 8
        == lax.broadcasted_iota(jnp.int32, (24, COLS * LANES), 1) // LANES
    ).astype(jnp.float32).astype(jnp.bfloat16)

    def graded(flag):
        return [soft_base + (soft_alpha * lam) * flag, 1.0 - lam * flag]

    deep = lax.broadcasted_iota(jnp.int32, (8, LANES), 0)
    def own_side():
        for q in range(blocks):
            rows = params[own_slot * blocks + q]
            rows = jnp.concatenate([rows[0:5], rows[5:6] * (0.5 * coulomb), rows[6:8]], axis=0)
            cols = thirds(rows).T.astype(jnp.bfloat16)
            wide = jnp.dot(cols, picks, preferred_element_type=jnp.float32)
            for r in range(7):
                own_cols[q, r] = wide[:, r * LANES : (r + 1) * LANES]
            for r, col in enumerate(graded(own_cols[q, 6])):
                own_cols[q, 7 + r] = col
            flag = rows[6:7]
            (soft,) = graded(flag)[:1]
            ratio = 1.0 / soft
            root = lax.rsqrt(soft)
            plain = params[own_slot * blocks + q][5:6]
            electric = (coulomb * root) * plain * plain
            first = rows[4:5] * rows[4:5] * ratio
            second = first * ratio
            alone = second - first
            slope = (second + alone) * ratio + 0.5 * electric * (root * root)
            alone = alone + electric
            for k, value in enumerate((alone, flag * alone, flag * slope)):
                self_ref[q, k] = jnp.where(deep == 0, value, 0.0)

    for q in range(blocks):
        for k in range(3):
            force_acc[q, k] = jnp.zeros((LANES, LANES), jnp.float32)

    def arrive(a, b):
        here = slot((a, b, 0))
        passing(own, (a, b, 0), here, 0).wait_recv()
        for c in up:
            sends.append(passing(ghost_ref.at[here], (0, 0, -c), slot((a, b, c)), len(sends)))
            sends[-1].start()

    def across(a, b):
        for c in up:
            passing(own, (0, 0, -c), slot((a, b, c)), 0).wait_recv()
            prepare(a, b, c)

    nearest = sides[::-1]
    prepare(0, 0, 0)
    for b in nearest:
        if b:
            arrive(0, b)
            prepare(0, b, 0)
    across(0, 0)
    for a in reach[1:]:
        for b in nearest:
            arrive(a, b)
            prepare(a, b, 0)
    for b in nearest:
        if b:
            across(0, b)
    for a in reach[1:]:
        for b in nearest:
            across(a, b)
    for o in ends:
        far_copy(0, o, far_slot(*o)).wait_recv()
    for a in reach[1:]:
        for b in nearest:
            for c in steps_of(nz):
                patch(a, b, c)
    for a in reach[:1]:
        for b in nearest:
            arrive(a, b)
    for b in nearest:
        for a in reach[:1]:
            prepare(a, b, 0)
            patch(a, b, 0)
        patch(0, b, 0)
    own_side()
    for b in nearest:
        for a in reach[:1]:
            across(a, b)
        for c in up:
            for a in [0] + reach[:1]:
                patch(a, b, c)

    width = listed_ref.shape[-1]
    together = 1 if width % 1 == 0 else 1
    groups = 16 if width % (16 * together) == 0 else 1

    def listed_rows(q, e):
        listed = listed_ref[q, 0, e]
        image = lax.div(listed, blocks)
        a = lax.div(image, 9) - 1
        b = lax.rem(lax.div(image, 3), 3) - 1
        c = lax.rem(image, 3) - 1
        where_from = (
            slot_step(a, nx) * len(steps_of(ny)) + slot_step(b, ny)
        ) * len(steps_of(nz)) + slot_step(c, nz)
        other = params[where_from * blocks + lax.rem(listed, blocks)]
        return other, [x.astype(jnp.float32) * y for x, y in zip((a, b, c), edge)], listed

    def entry(q, e):
        other, step_by, listed = listed_rows(q, e)
        left = jnp.minimum(jnp.maximum(count_ref[0, 0, 0, q] - e, 0), 1)
        used = left.astype(jnp.float32)
        apart = jnp.abs(listed - (13 * blocks + q))
        itself = ((1 - jnp.minimum(apart, 1)) * left).astype(jnp.float32)
        rows = []
        for r in range(7):
            row = other[r : r + 1]
            if r < 3:
                row = row + step_by[r]
            if 4 <= r < 6:
                row = row * used
            rows.append(row)
        rows.append(graded(rows[6])[0])
        return [jnp.broadcast_to(row, (8, LANES)) for row in rows], itself

    def turn(q, step):
        others = [entry(q, step * together + k) for k in range(together)]
        tot, tot_p, tot_k = (
            sum(-itself * self_ref[q, k] for _, itself in others) for k in range(3)
        )
        for g in range(LANES // 8):
            at = pl.ds(g * 8, 8)
            xi, yi, zi, hi, ei, qi, pi, si = (own_cols[q, r, at] for r in range(8))
            for k, ((xj, yj, zj, hj, ej, qj, pj, sj), _) in enumerate(others):
                dx, dy, dz = xi - xj, yi - yj, zi - zj
                r2 = dx * dx + dy * dy + dz * dz
                sig = hi + hj
                is2 = 1.0 / (sig * sig)
                soft = jnp.maximum(si, sj)
                p = jnp.maximum(pi, pj)
                x = r2 * is2
                x2 = x * x
                t = 1.0 / (soft + x2 * x)
                u = lax.rsqrt(3.0 * r2 + soft)
                half = (qi * qj) * u
                ec = half + half
                half = half * (u * u)
                first = (ei * ej) * t
                second = first * t
                v = second - first
                mt = (second + v) * t
                v = v + ec
                kk = mt + half
                slopes[q, step * together + k, at] = mt * (x2 * is2) + half
                tot = tot + v
                tot_p = tot_p + p * v
                tot_k = tot_k + p * kk
        for k, value in enumerate((tot, tot_p, tot_k)):
            sums_ref[k] += value

    joined_blocks = 2 if blocks % 2 == 0 else 1

    @pl.loop(0, blocks // joined_blocks)
    def _(some):
        for k in range(joined_blocks):
            for step in range(width // together):
                turn(some * joined_blocks + k, step)

    part = LANES // 4

    def narrowed(row):
        row = row + pltpu.roll(row, LANES // 2, 1)
        return row + pltpu.roll(row, part, 1)

    folded = [narrowed(jnp.sum(sums_ref[k], axis=0, keepdims=True)) for k in range(3)]
    lane = lax.broadcasted_iota(jnp.int32, (1, LANES), 1)
    mine = jnp.where(lane < part, folded[0], jnp.where(lane < 2 * part, folded[1], folded[2]))
    tile[...] = mine
    gathered[my_id] = mine

    def share(by):
        return pltpu.make_async_remote_copy(
            src_ref=tile,
            dst_ref=gathered.at[my_id],
            send_sem=sum_send.at[by],
            recv_sem=sum_recv.at[by],
            device_id=window_device(lax.rem(my_id + by, total)),
            device_id_type=MESH,
        )

    if total <= 32:
        for by in range(1, total):
            share(by).start()
    else:

        @pl.loop(1, total)
        def _(by):
            share(by).start()

    joint = 4 if width % 4 == 0 else 1

    @pl.loop(0, blocks)
    def _(q):
        def sweep(step):
            others = []
            for k in range(joint):
                other, step_by, _ = listed_rows(q, step * joint + k)
                rows = [other[r : r + 1] + step_by[r] for r in range(3)]
                rows.append(graded(other[6:7])[1])
                others.append([jnp.broadcast_to(row, (8, LANES)) for row in rows])
            for g in range(LANES // 8):
                at = pl.ds(g * 8, 8)
                xi, yi, zi, wi = (own_cols[q, r, at] for r in (0, 1, 2, 8))
                forces = None
                for k, (xj, yj, zj, wj) in enumerate(others):
                    fs = slopes[q, step * joint + k, at] * jnp.minimum(wi, wj)
                    new = [fs * (xi - xj), fs * (yi - yj), fs * (zi - zj)]
                    forces = new if forces is None else [x + y for x, y in zip(forces, new)]
                for k in range(3):
                    force_acc[q, k, at] += forces[k]

        for step in range(width // joint):
            sweep(step)

    for q in range(blocks):
        for k in range(3):
            whole = force_acc[q, k]
            high = whole.astype(jnp.bfloat16)
            low = (whole - high.astype(jnp.float32)).astype(jnp.bfloat16)
            reduced = sum(
                lax.dot_general(
                    ones, part, (((1,), (1,)), ((), ())), preferred_element_type=jnp.float32
                )
                for part in (high, low)
            )
            force_ref[k, 0, 0, :, q * LANES : (q + 1) * LANES] = (2.0 * 3.0**0.5) * reduced[0:1]

    for copy in sends + far_copies:
        copy.wait_send()

    @pl.loop(1, total)
    def _(by):
        share(by).wait()

    summed = jnp.sum(gathered[...], axis=0)
    third = lax.div(lane, part)
    scale = 0.5 / float(atoms * total)
    first = jnp.where(third == 0, scale, jnp.where(third == 1, -scale * lam, 0.0))
    second = jnp.where(third == 1, -scale, (-0.5 * scale) * (1.0 - lam))
    second = jnp.where(third == 0, 0.0, jnp.where(third == 3, 0.0, second))
    both = jnp.concatenate([summed * first, summed * second], axis=0)
    tally_ref[...] = jnp.broadcast_to(jnp.sum(both, axis=1, keepdims=True), (2, LANES))


def hand_over(force_in, tally_in, force_ref, energy_ref, dhdl_ref, sem):
    copy = pltpu.make_async_copy(force_in, force_ref, sem)
    copy.start()
    energy_ref[0] = tally_in[0, 0]
    dhdl_ref[0] = tally_in[1, 0]
    copy.wait()


def on_device(sizes, fraction, atom_type, perturbed, leaving, neighbours, counts,
              sigma_table, depth_table, charge_table, domain_edge, coupling):
    nx, ny, nz = sizes
    atoms = fraction.shape[-1]
    mig = leaving.shape[-1]
    slots = len(steps_of(nx)) * len(steps_of(ny)) * len(steps_of(nz))
    planar = len(steps_of(ny)) * len(steps_of(nz))
    far_slots = max(len(far_steps(nx)), 1) * planar
    extras = -(-(ROWS + 1) // (LANES // (2 * mig)))
    smem = pl.BlockSpec(memory_space=pltpu.SMEM)
    vmem = pl.BlockSpec(memory_space=pltpu.VMEM)
    f32 = jnp.float32

    def bound(kernel, *values):
        return lambda *refs: kernel(*values, *refs)

    blocks = atoms // LANES
    total = nx * ny * nz
    dma = pltpu.SemaphoreType.DMA
    arrays = (
        domain_edge,
        coupling,
        sigma_table,
        depth_table,
        charge_table,
        neighbours.reshape(blocks, 1, -1),
        counts,
        fraction,
        atom_type,
        perturbed,
        leaving,
    )
    forces, tally = pl.pallas_call(
        bound(step_kernel, sizes),
        name="step",
        out_shape=(pltpu.VMEM(fraction.shape, f32), pltpu.VMEM((2, LANES), f32)),
        in_specs=[pl.BlockSpec(memory_space=pl.ANY)] * 11,
        out_specs=(vmem, vmem),
        scratch_shapes=[
            *(pltpu.SMEM(x.shape, x.dtype) for x in arrays[:7]),
            *(pltpu.VMEM(x.shape, x.dtype) for x in arrays[7:]),
            dma((11,)),
            pltpu.VMEM((slots, blocks * ROWS + extras, 1, LANES), f32),
            pltpu.VMEM((far_slots, extras, 1, LANES), f32),
            pltpu.VMEM((slots, 2 * mig, atoms), jnp.bfloat16),
            pltpu.VMEM((blocks, COLS, LANES, LANES), f32),
            pltpu.VMEM((blocks, 3, LANES, LANES), f32),
            pltpu.VMEM((slots * blocks, 8, LANES), f32),
            pltpu.VMEM((blocks, 3, 8, LANES), f32),
            pltpu.VMEM((blocks, neighbours.shape[-1], LANES, LANES), f32),
            pltpu.VMEM((3, 8, LANES), f32),
            pltpu.VMEM((1, LANES), f32),
            pltpu.VMEM((total, 1, LANES), f32),
            dma((far_slots,)),
            dma((far_slots,)),
            dma((slots,)),
            dma((slots,)),
            dma((total,)),
            dma((total,)),
        ],
        compiler_params=pltpu.CompilerParams(collective_id=0, has_side_effects=True),
    )(*arrays)
    return pl.pallas_call(
        hand_over,
        name="hand_over",
        out_shape=(
            jax.ShapeDtypeStruct(fraction.shape, f32),
            jax.ShapeDtypeStruct((1,), f32),
            jax.ShapeDtypeStruct((1,), f32),
        ),
        in_specs=[vmem, vmem],
        out_specs=(pl.BlockSpec(memory_space=pl.ANY), smem, smem),
        scratch_shapes=[pltpu.SemaphoreType.DMA],
    )(pltpu.with_memory_space_constraint(forces, pltpu.VMEM), pltpu.with_memory_space_constraint(tally, pltpu.VMEM))


def solution(mesh):
    sizes = (mesh.shape["dx"], mesh.shape["dy"], mesh.shape["dz"])
    return jax.shard_map(
        lambda *arrays: on_device(sizes, *arrays),
        mesh=mesh,
        in_specs=(
            P(None, ("win", "dx"), "dy", "dz", None),
            P(("win", "dx"), "dy", "dz", None),
            P(("win", "dx"), "dy", "dz", None),
            P(("win", "dx"), "dy", "dz", None, None),
            P(("win", "dx"), "dy", "dz", None, None),
            P(("win", "dx"), "dy", "dz", None),
            P(),
            P(),
            P(),
            P(),
            P("win"),
        ),
        out_specs=(P(None, ("win", "dx"), "dy", "dz", None), P("win"), P("win")),
        check_vma=False,
    )
```
